32 devices in a mesh: dp: 8 (over y, x, core), tensor: 4 (over z).
Axes of the slice: x: 2, y: 2, z: 4, core: 2. Of those that a mesh axis runs over, the one named last changes fastest.
Arguments:
- layer_input: float32 [16, 512, 2048], P('dp', 'tensor'), may hold values from -6 to 6
- segments: int32 [16, 512], P('dp'), may hold values from 0 to 7, never falling along the last dimension, each value on 1 to 256 neighbouring positions
- gain_attn: bfloat16 [2048], P('dp'), may hold values from 0.5 to 1.5
- w_qkv: bfloat16 [2048, 4, 640], P('dp', 'tensor'), as said below
- w_out_t: bfloat16 [2048, 2048], P('dp', 'tensor'), may hold values from -0.75 to 0.75
- gain_mlp: bfloat16 [2048], P('dp'), may hold values from 0.5 to 1.5
- w_gate_up: bfloat16 [2048, 2, 5632], P('dp', None, 'tensor'), may hold values from -0.125 to 0.125
- w_down_t: bfloat16 [2048, 5632], P('dp', 'tensor'), may hold values from -0.078125 to 0.078125
- cotangent: float32 [16, 512, 2048], P('dp', 'tensor'), may hold values from -6 to 6
Outputs:
- output: float32 [16, 512, 2048], P('dp', 'tensor')
- input_grad: float32 [16, 512, 2048], P('dp', 'tensor')
- gain_attn_grad: float32 [2048], P('dp')
- qkv_grad: float32 [2048, 4, 640], P('dp', 'tensor')
- out_grad: float32 [2048, 2048], P('dp', 'tensor')
- gain_mlp_grad: float32 [2048], P('dp')
- gate_up_grad: float32 [2048, 2, 5632], P('dp', None, 'tensor')
- down_grad: float32 [2048, 5632], P('dp', 'tensor')
The draws below stay inside these ranges and needn't reach their ends.
Inputs may be any that keep to these rules, and one draw needn't show every extreme that they name: `w_qkv`: for each key-value group the columns hold the queries of its 8 heads, then its key, then its value.
All inputs are finite; a program needn't handle non-finite values.
Results may differ from the reference program's by a relative error of at most 0.013.
Values may be sent and summed in bfloat16 or wider, within the bound.
A program may use at most 256 MiB of HBM per device.

```python
import math
import jax
import jax.numpy as jnp
import numpy as np
from jax import lax

D = 2048
H = 32
KV = 4
HD = 64
FF = 5632
ROWS = 512
SEGS = 8
NBLK = 16


def draw_w_qkv(key, part):
    head_group = H // KV
    base_draw = jax.random.truncated_normal(key, -5.0, 5.0, (D, KV, (head_group + 2) * HD), jnp.float32) * (1.0 / math.sqrt(D))
    return base_draw.astype(jnp.bfloat16)


def with_spikes(values, stream_key, source, target, blocks, factor):
    owner, partner = [(jnp.arange(values.shape[dim]) // (values.shape[dim] // blocks)).reshape([-1 if axis == dim else 1 for axis in range(values.ndim)]) for dim in (source, target)]
    chosen = jax.random.permutation(stream_key, blocks)[partner]
    strong = (owner == chosen) | (owner == (partner + blocks // 2) % blocks)
    return jnp.where(strong, factor * values, values)


def level_of(rng, shape, split, least, top_value):
    def one(dim, shards_of):
        draws = jax.random.uniform(jax.random.fold_in(jax.random.fold_in(rng, 6), dim), (shards_of,), jnp.float32, least / len(split), top_value / len(split))
        return jnp.repeat(jnp.exp(draws), shape[dim] // shards_of).reshape((-1,) + (1,) * (len(shape) - dim - 1))

    loudness = one(*split[0])
    for cut in split[1:]:
        loudness = loudness * one(*cut)
    return loudness


def length_profile(number_of, total, limit, slope):
    weights = [(1 << 20) // math.isqrt(grade ** slope) + 1 for grade in range(2, number_of + 1)]
    spare, given = total - limit - (number_of - 1), [1] * (number_of - 1)
    while spare > 0:
        candidates = [i for i in range(number_of - 1) if given[i] < limit]
        mass, remaining = sum([weights[i] for i in candidates]), spare
        for i in candidates:
            extra = min(limit - given[i], max(1, remaining * weights[i] // mass), spare)
            given[i] = given[i] + extra
            spare = spare - extra
    return np.array([limit] + given)


def uneven(stream_key, count, total, limit, slope):
    if count == 2:
        one = jax.random.randint(stream_key, (), max(1, total - limit), min(limit, total - 1) + 1)
        return jnp.stack([one, total - one])
    lengths = jnp.asarray(length_profile(count, total, limit, slope), jnp.int32)
    pairs = (count - 1) // 2
    source_of, receiver = lengths[1:1 + 2 * pairs:2], lengths[2:2 + 2 * pairs:2]
    room = jnp.minimum(source_of - 1, limit - receiver)
    shifted = jax.random.randint(jax.random.fold_in(stream_key, 1), (pairs,), 0, 1 << 20) % (room + 1)
    lengths = lengths.at[1:1 + 2 * pairs:2].set(source_of - shifted).at[2:2 + 2 * pairs:2].set(receiver + shifted)
    return lengths[jax.random.permutation(jax.random.fold_in(stream_key, 2), count)]


def bell_draw(rng, dims, width, reach, split=(), kind=jnp.bfloat16):
    array = width * jax.random.normal(rng, dims, jnp.float32)
    if split:
        array = array * level_of(rng, dims, split, -0.22, 0.18)
    return jnp.clip(array, -reach, reach).astype(kind)


def noise_with(stream_key, extent, spread, bound, split, heavy, held_as=jnp.bfloat16):
    array = spread * jax.random.normal(stream_key, extent, jnp.float32)
    if split:
        array = array * level_of(stream_key, extent, split, -0.22, 0.18)
    return jnp.clip(with_spikes(array, jax.random.fold_in(stream_key, 3), *heavy), -bound, bound).astype(held_as)


def setup_inputs(seed: int = 0) -> dict:
    splits = jax.random.split(jax.random.key(seed), 10)
    return {
        "layer_input": bell_draw(splits[0], (NBLK, ROWS, D), 1.0, 6.0, ((0, 8), (1, 4)), jnp.float32),
        "segments": jax.vmap(lambda own: jnp.searchsorted(jnp.cumsum(uneven(own, SEGS, ROWS, ROWS // 2, 2)), jnp.arange(ROWS), side="right"))(jax.random.split(splits[1], NBLK)).reshape((NBLK, ROWS)).astype(jnp.int32),
        "gain_attn": jnp.clip(1.0 + 0.1 * jax.random.normal(splits[2], (D,), jnp.float32), 0.5, 1.5).astype(jnp.bfloat16),
        "w_qkv": draw_w_qkv(jax.random.fold_in(splits[9], 71), 0),
        "w_out_t": bell_draw(splits[4], (D, H * HD), (H * HD // 32) ** -0.5, 0.75, ((0, 8), (1, 4))),
        "gain_mlp": jnp.clip(1.0 + 0.1 * jax.random.normal(splits[5], (D,), jnp.float32), 0.5, 1.5).astype(jnp.bfloat16),
        "w_gate_up": bell_draw(splits[6], (D, 2, FF), D ** -0.5, 0.125, ((0, 8), (2, 4))),
        "w_down_t": bell_draw(splits[7], (D, FF), FF ** -0.5, 0.078125, ((0, 8), (1, 4))),
        "cotangent": noise_with(splits[8], (NBLK, ROWS, D), 1.0, 6.0, ((0, 8), (1, 4)), (0, 2, 8, 2.0), jnp.float32),
    }


NORM_EPS = 1e-05

def rope_tables(segment_row, head_size):
    row_count = segment_row.shape[0]
    earlier = lax.optimization_barrier(jnp.sum((segment_row[None, :] < segment_row[:, None]).astype(jnp.int32), axis=1))
    position = (jnp.arange(row_count, dtype=jnp.int32) - earlier).astype(jnp.float32)
    half_size = head_size // 2
    frequency = jnp.exp(jnp.arange(half_size, dtype=jnp.float32) * (-2.0 * math.log(10000.0) / head_size))
    angles = position[:, None] * frequency[None, :]
    return (jnp.cos(angles), jnp.sin(angles))

def expand_table(angle_table, rank_count):
    return angle_table.reshape((angle_table.shape[0],) + (1,) * (rank_count - 2) + (angle_table.shape[1],))

def rotate(values, cosine, sine_tab):
    half_size = values.shape[-1] // 2
    cosine = expand_table(cosine, values.ndim)
    sine_tab = expand_table(sine_tab, values.ndim)
    first_half = values[..., :half_size]
    second_half = values[..., half_size:]
    return jnp.concatenate([first_half * cosine - second_half * sine_tab, second_half * cosine + first_half * sine_tab], axis=-1)

def unrotate(values, cosine, sine_tab):
    half_size = values.shape[-1] // 2
    cosine = expand_table(cosine, values.ndim)
    sine_tab = expand_table(sine_tab, values.ndim)
    first_half = values[..., :half_size]
    second_half = values[..., half_size:]
    return jnp.concatenate([first_half * cosine + second_half * sine_tab, second_half * cosine - first_half * sine_tab], axis=-1)

def allowed_pairs(segment_row):
    row_count = segment_row.shape[0]
    position = jnp.arange(row_count, dtype=jnp.int32)
    return (segment_row[:, None] == segment_row[None, :]) & (position[None, :] <= position[:, None])

def norm_forward(row_block, gain_row):
    inv_rms = lax.rsqrt(lax.optimization_barrier(jnp.mean(row_block * row_block, axis=-1, keepdims=True)) + NORM_EPS)
    return ((row_block * inv_rms * gain_row.astype(jnp.float32)).astype(jnp.bfloat16), inv_rms)

def norm_backward(row_block, inv_rms, gain_row, upstream):
    weighted = upstream * gain_row.astype(jnp.float32)
    back_term = inv_rms * weighted - row_block * (inv_rms * inv_rms * inv_rms) * lax.optimization_barrier(jnp.mean(weighted * row_block, axis=-1, keepdims=True))
    return (back_term, lax.optimization_barrier(jnp.sum(upstream * row_block * inv_rms, axis=0)))

def split_heads(qkv_rows, head_group, head_size):
    row_count, groups = (qkv_rows.shape[0], qkv_rows.shape[1])
    query = qkv_rows[:, :, :head_group * head_size].reshape(row_count, groups, head_group, head_size)
    key_part = qkv_rows[:, :, head_group * head_size:(head_group + 1) * head_size]
    value_part = qkv_rows[:, :, (head_group + 1) * head_size:]
    return (query, key_part, value_part)

def score_block(query, key_part, allowed, head_size):
    scores = jnp.einsum('igne,jge->gnij', query.astype(jnp.float32), key_part.astype(jnp.float32)) * (1.0 / math.sqrt(head_size))
    return jnp.where(allowed[None, None], scores, jnp.float32(-1e+30))

def attend_forward(qkv_rows, segment_row, head_group, head_size):
    cosine, sine_tab = rope_tables(segment_row, head_size)
    query, key_part, value_part = split_heads(qkv_rows, head_group, head_size)
    query = rotate(query, cosine, sine_tab).astype(jnp.bfloat16)
    key_part = rotate(key_part, cosine, sine_tab).astype(jnp.bfloat16)
    value_part = value_part.astype(jnp.bfloat16)
    allowed = allowed_pairs(segment_row)
    scores = score_block(query, key_part, allowed, head_size)
    row_max = lax.optimization_barrier(jnp.max(scores, axis=-1, keepdims=True))
    log_total = row_max + jnp.log(lax.optimization_barrier(jnp.sum(jnp.exp(scores - row_max), axis=-1, keepdims=True)))
    weights = jnp.exp(scores - log_total).astype(jnp.bfloat16)
    mixed = jnp.einsum('gnij,jge->igne', weights.astype(jnp.float32), value_part.astype(jnp.float32))
    mixed = mixed.astype(jnp.bfloat16).reshape(qkv_rows.shape[0], -1)
    return (mixed, (query, key_part, value_part, log_total, cosine, sine_tab, allowed))

def attend_backward(grad_out, saved, head_size):
    query, key_part, value_part, log_total, cosine, sine_tab, allowed = saved
    row_count, groups, head_group = (query.shape[0], query.shape[1], query.shape[2])
    scores = score_block(query, key_part, allowed, head_size)
    weights = jnp.exp(scores - log_total)
    grad_heads = grad_out.reshape(row_count, groups, head_group, head_size).astype(jnp.float32)
    grad_value = jnp.einsum('gnij,igne->jge', weights.astype(jnp.bfloat16).astype(jnp.float32), grad_heads)
    grad_weights = jnp.einsum('igne,jge->gnij', grad_heads, value_part.astype(jnp.float32))
    grad_scores = weights * (grad_weights - lax.optimization_barrier(jnp.sum(weights * grad_weights, axis=-1, keepdims=True))) * (1.0 / math.sqrt(head_size))
    grad_scores = grad_scores.astype(jnp.bfloat16).astype(jnp.float32)
    grad_query = jnp.einsum('gnij,jge->igne', grad_scores, key_part.astype(jnp.float32))
    grad_key = jnp.einsum('gnij,igne->jge', grad_scores, query.astype(jnp.float32))
    grad_query = unrotate(grad_query, cosine, sine_tab).reshape(row_count, groups, head_group * head_size)
    grad_key = unrotate(grad_key, cosine, sine_tab)
    return jnp.concatenate([grad_query, grad_key, grad_value], axis=2).astype(jnp.bfloat16)

def reference(layer_input, segments, gain_attn, w_qkv, w_out_t, gain_mlp, w_gate_up, w_down_t, cotangent):
    head_group = H // KV
    qkv_flat = w_qkv.reshape(D, -1)
    gu_flat = w_gate_up.reshape(D, -1)

    def micro_step(state_acc, item_data):
        rows_in, segment_row, grad_in = item_data
        normed_attn, scale_attn = norm_forward(rows_in, gain_attn)
        qkv_rows = jnp.dot(normed_attn, qkv_flat, preferred_element_type=jnp.float32).reshape(ROWS, KV, -1)
        mixed, saved = attend_forward(qkv_rows, segment_row, head_group, HD)
        residual = rows_in + jnp.dot(mixed, w_out_t.T, preferred_element_type=jnp.float32)
        normed_mlp, scale_mlp = norm_forward(residual, gain_mlp)
        gate_up = jnp.dot(normed_mlp, gu_flat, preferred_element_type=jnp.float32).reshape(ROWS, 2, FF)
        gate_part = gate_up[:, 0]
        up_part = gate_up[:, 1]
        sigmoid_gate = jax.nn.sigmoid(gate_part)
        active = gate_part * sigmoid_gate
        hidden = (active * up_part).astype(jnp.bfloat16)
        output_rows = residual + jnp.dot(hidden, w_down_t.T, preferred_element_type=jnp.float32)
        grad_rows = grad_in.astype(jnp.bfloat16)
        grad_down = jnp.dot(grad_rows.T, hidden, preferred_element_type=jnp.float32)
        grad_hidden = jnp.dot(grad_rows, w_down_t, preferred_element_type=jnp.float32)
        grad_gu = jnp.stack([grad_hidden * up_part * sigmoid_gate * (1.0 + gate_part * (1.0 - sigmoid_gate)), grad_hidden * active], axis=1).astype(jnp.bfloat16)
        flat_gu = grad_gu.reshape(ROWS, -1)
        grad_gu_w = jnp.dot(normed_mlp.T, flat_gu, preferred_element_type=jnp.float32).reshape(D, 2, FF)
        grad_normed_mlp = jnp.dot(flat_gu, gu_flat.T, preferred_element_type=jnp.float32)
        back_mlp, grad_g_mlp = norm_backward(residual, scale_mlp, gain_mlp, grad_normed_mlp)
        grad_resid = grad_in + back_mlp
        resid_rows = grad_resid.astype(jnp.bfloat16)
        grad_out_w = jnp.dot(resid_rows.T, mixed, preferred_element_type=jnp.float32)
        grad_mixed = jnp.dot(resid_rows, w_out_t, preferred_element_type=jnp.float32).astype(jnp.bfloat16)
        grad_qkv = attend_backward(grad_mixed, saved, HD)
        flat_qkv = grad_qkv.reshape(ROWS, -1)
        grad_qkv_w = jnp.dot(normed_attn.T, flat_qkv, preferred_element_type=jnp.float32).reshape(w_qkv.shape)
        grad_normed_attn = jnp.dot(flat_qkv, qkv_flat.T, preferred_element_type=jnp.float32)
        back_attn, grad_g_attn = norm_backward(rows_in, scale_attn, gain_attn, grad_normed_attn)
        new_terms = (grad_g_attn, grad_qkv_w, grad_out_w, grad_g_mlp, grad_gu_w, grad_down)
        state_acc = tuple((left_term + right_term for left_term, right_term in zip(state_acc, new_terms)))
        return (state_acc, (output_rows, grad_resid + back_attn))
    start_acc = (jnp.zeros((D,), jnp.float32), jnp.zeros(w_qkv.shape, jnp.float32), jnp.zeros(w_out_t.shape, jnp.float32), jnp.zeros((D,), jnp.float32), jnp.zeros(w_gate_up.shape, jnp.float32), jnp.zeros(w_down_t.shape, jnp.float32))
    final_acc, stacked = lax.scan(micro_step, start_acc, (layer_input, segments, cotangent))
    return (stacked[0], stacked[1], final_acc[0], final_acc[1], final_acc[2], final_acc[3], final_acc[4], final_acc[5])
```

```python
import functools
import math

import jax
import jax.numpy as jnp
from jax import lax
from jax.experimental import pallas as pl
from jax.experimental.pallas import tpu as pltpu
from jax.sharding import PartitionSpec as P

HD = 64
NORM_EPS = 1e-05
F32 = jnp.float32
BF16 = jnp.bfloat16
MESH = pl.DeviceIdType.MESH
LATE = 2


class Cube:
    def __init__(self, size):
        self.size = size
        self.bits = size.bit_length() - 1
        assert 1 << self.bits == size and self.bits >= 1
        self.shape = (2,) * self.bits
        outer = list(range(1, self.bits))
        self.steps = len(outer)
        self.parts = max(1, self.steps)
        self.orders = [outer[p:] + outer[:p] for p in range(self.parts)]

    def own(self, bit):
        return lax.axis_index("dp") // (1 << bit) % 2

    def partner(self, bit):
        return lax.axis_index("dp") + (1 << bit) * (1 - 2 * self.own(bit))

    def index(self, free, flipped=()):
        spots = []
        for bit in reversed(range(self.bits)):
            if bit in free:
                spots.append(slice(None))
            else:
                spots.append(1 - self.own(bit) if bit in flipped else self.own(bit))
        return tuple(spots)

    def cuts(self, rows):
        count = rows // self.parts
        return [pl.ds(part * count, count) for part in range(self.parts)]

    def move(self, step, part):
        if step == self.steps:
            return tuple(range(1, self.bits)), 0
        return tuple(self.orders[part][:step]), self.orders[part][step]

    def keys(self, step):
        return [(step, part) for part in range(self.parts if step < self.steps else 1)]

    def row(self, key):
        return key[0] * self.parts + key[1]


class Gather:
    def __init__(self, kinds, late, shapes, n_t, n_dp, ident):
        self.kinds, self.late, self.shapes = kinds, late, shapes
        self.n_t, self.cube, self.ident = n_t, Cube(n_dp), ident
        self.ticks = [[("own", 0)]] + [[("up", k), ("down", k)] for k in range(1, n_t)]
        self.insts = [inst for tick in self.ticks for inst in tick]
        self.uses_dp = any("d" in kind for kind in kinds)
        self.uses_z = any("z" in kind for kind in kinds)
    def out_shape(self, a):
        rows, cols = self.shapes[a]
        kind = self.kinds[a]
        if kind == "z":
            return (self.n_t, rows, cols)
        return self.cube.shape + (rows, cols * (self.n_t if "z" in kind else 1))

    def place(self, ref, a, z, free=(), flipped=(), part=None):
        rows, cols = self.shapes[a]
        kind = self.kinds[a]
        if kind == "z":
            return ref.at[z]
        span = pl.ds(0, rows) if part is None else self.cube.cuts(rows)[part]
        width = pl.ds(pl.multiple_of(z * cols, cols), cols) if "z" in kind else pl.ds(0, cols)
        return ref.at[self.cube.index(free, flipped) + (span, width)]

    def kernel(self, *refs):
        count = len(self.kinds)
        srcs, dests = refs[:count], refs[count : 2 * count]
        own_sem, z_send, z_recv, d_send, d_recv = refs[2 * count :]
        n_t, cube = self.n_t, self.cube
        me_t = lax.axis_index("tensor")
        main = [a for a in range(count) if not self.late[a]]
        tail = [a for a in range(count) if self.late[a]]

        barrier = pltpu.get_barrier_semaphore()
        if self.uses_dp:
            for bit in range(cube.bits):
                pl.semaphore_signal(barrier, inc=1, device_id={"dp": cube.partner(bit)}, device_id_type=MESH)
        peers = self.n_t - 1 if self.uses_z else 0
        for r in range(peers):
            pl.semaphore_signal(barrier, inc=1, device_id={"tensor": (me_t + 1 + r) % n_t}, device_id_type=MESH)
        pl.semaphore_wait(barrier, peers + (cube.bits if self.uses_dp else 0))

        def own_copy(a):
            return pltpu.make_async_copy(srcs[a], self.place(dests[a], a, me_t), own_sem.at[a])

        for a in range(count):
            own_copy(a).start()

        def piece_of(inst):
            way, k = inst
            return me_t if way == "own" else me_t - k if way == "up" else me_t + k

        def exists(inst, fn):
            way, k = inst
            if way == "own":
                fn()
            elif way == "up":
                pl.when(me_t >= k)(fn)
            else:
                pl.when(me_t + k < n_t)(fn)

        def z_copy(a, way, k, src):
            piece = me_t - (k - 1) if way == "up" else me_t + (k - 1)
            index = 2 * (k - 1) + (way == "down")
            dest = self.place(dests[a], a, piece)
            return pltpu.make_async_remote_copy(
                src_ref=dest if src is None else src,
                dst_ref=dest,
                send_sem=z_send.at[a, index],
                recv_sem=z_recv.at[a, index],
                device_id={"tensor": me_t + 1 if way == "up" else me_t - 1},
                device_id_type=MESH,
            )

        def z_cond(way, k):
            return (
                jnp.logical_and(me_t >= k - 1, me_t < n_t - 1)
                if way == "up"
                else jnp.logical_and(me_t + (k - 1) < n_t, me_t > 0)
            )

        def z_start(a, inst):
            way, k = inst
            for out_way in ("up", "down") if way == "own" else (way,):
                if k + 1 < n_t:

                    @pl.when(z_cond(out_way, k + 1))
                    def _():
                        z_copy(a, out_way, k + 1, srcs[a] if way == "own" else None).start()

        def z_arrive(a, inst):
            way, k = inst
            if way != "own":
                index = 2 * (k - 1) + (way == "down")
                dest = self.place(dests[a], a, piece_of(inst))
                pltpu.make_async_remote_copy(
                    src_ref=dest,
                    dst_ref=dest,
                    send_sem=z_send.at[a, index],
                    recv_sem=z_recv.at[a, index],
                    device_id={"tensor": me_t},
                    device_id_type=MESH,
                ).wait_recv()

        def d_copy(a, inst, key, incoming=False):
            free, bit = cube.move(*key)
            part = key[1] if key[0] < cube.steps else None
            spot = self.place(dests[a], a, piece_of(inst), free, (bit,) if incoming else (), part)
            sem = (a, self.insts.index(inst), cube.row(key))
            return pltpu.make_async_remote_copy(
                src_ref=spot,
                dst_ref=spot,
                send_sem=d_send.at[sem],
                recv_sem=d_recv.at[sem],
                device_id={"dp": cube.partner(bit)},
                device_id_type=MESH,
            )

        def d_advance(a, inst, stage):
            if stage == 0 and inst[0] == "own":
                own_copy(a).wait()
            if stage > 0:
                for key in cube.keys(stage - 1):
                    d_copy(a, inst, key, True).wait_recv()
            if stage <= cube.steps:
                for key in cube.keys(stage):
                    d_copy(a, inst, key).start()

        def in_dp(a, inst):
            return "d" in self.kinds[a] and (inst[0] == "own" or "z" in self.kinds[a])

        z_main = [a for a in main if "z" in self.kinds[a]]
        z_tail = [a for a in tail if "z" in self.kinds[a]]
        length = n_t if self.uses_z else 1
        total = max(length + cube.steps + 2, 2 * length + 1)
        for now in range(total):
            for inst in self.ticks[now] if now < length else ():
                def arrive(inst=inst):
                    for a in z_main:
                        z_arrive(a, inst)
                        z_start(a, inst)
                    for a in main:
                        if in_dp(a, inst):
                            d_advance(a, inst, 0)

                exists(inst, arrive)
            late_now = now - length + LATE
            if 0 <= late_now < length and z_tail:
                for inst in self.ticks[late_now]:
                    def arrive_late(inst=inst):
                        for a in z_tail:
                            z_arrive(a, inst)
                            z_start(a, inst)

                    exists(inst, arrive_late)
            for age in range(1, cube.steps + 2):
                tick = now - age
                for inst in self.ticks[tick] if 0 <= tick < length else ():
                    def advance(inst=inst, age=age):
                        for a in main:
                            if in_dp(a, inst):
                                d_advance(a, inst, age)

                    exists(inst, advance)

        for inst in self.insts:
            def drain(inst=inst):
                for a in main:
                    if in_dp(a, inst):
                        for stage in range(cube.steps + 1):
                            for key in cube.keys(stage):
                                d_copy(a, inst, key).wait_send()

            exists(inst, drain)
        for a in range(count):
            if "z" in self.kinds[a]:
                for k in range(1, n_t):
                    for way in ("up", "down"):

                        @pl.when(z_cond(way, k))
                        def _():
                            z_copy(a, way, k, srcs[a] if k == 1 else None).wait_send()

            if not in_dp(a, ("own", 0)):
                own_copy(a).wait()

    def __call__(self, *arrays):
        count = len(arrays)
        n_z = max(1, 2 * (self.n_t - 1))
        rows = (self.cube.steps + 1) * self.cube.parts
        insts = len(self.insts) if self.uses_dp else 1
        outs = pl.pallas_call(
            self.kernel,
            out_shape=[jax.ShapeDtypeStruct(self.out_shape(a), arrays[a].dtype) for a in range(count)],
            in_specs=[pl.BlockSpec(memory_space=pltpu.VMEM)] * count,
            out_specs=[pl.BlockSpec(memory_space=pl.ANY)] * count,
            scratch_shapes=[
                pltpu.SemaphoreType.DMA((count,)),
                pltpu.SemaphoreType.DMA((count, n_z)),
                pltpu.SemaphoreType.DMA((count, n_z)),
                pltpu.SemaphoreType.DMA((count, insts, rows)),
                pltpu.SemaphoreType.DMA((count, insts, rows)),
            ],
            compiler_params=pltpu.CompilerParams(collective_id=self.ident, has_side_effects=True),
        )(*arrays)
        return [
            out.reshape(-1, out.shape[-1]) if "d" in kind else out for out, kind in zip(outs, self.kinds)
        ]


class Scatter:
    def __init__(self, kinds, pieces, n_t, n_dp, ident):
        self.kinds = kinds
        self.pieces = [n_t if kind == "dz" else count for kind, count in zip(kinds, pieces)]
        self.n_t, self.cube, self.ident = n_t, Cube(n_dp), ident

    def kernel(self, *refs):
        count = len(self.kinds)
        n_t, cube = self.n_t, self.cube
        grads, outs = refs[:count], refs[count : 2 * count]
        core_in, z_in = refs[2 * count : 3 * count], refs[3 * count : 4 * count]
        step_in = [refs[4 * count + a * cube.steps :][: cube.steps] for a in range(count)]
        d_send, d_recv, z_send, z_recv = refs[-4:]
        me_t = lax.axis_index("tensor")
        to_z = any(kind != "d" for kind in self.kinds)

        barrier = pltpu.get_barrier_semaphore()
        for bit in range(cube.bits):
            pl.semaphore_signal(barrier, inc=1, device_id={"dp": cube.partner(bit)}, device_id_type=MESH)
        if to_z:
            for r in range(1, n_t):
                pl.semaphore_signal(barrier, inc=1, device_id={"tensor": (me_t + r) % n_t}, device_id_type=MESH)
        pl.semaphore_wait(barrier, cube.bits + (n_t - 1 if to_z else 0))

        def columns(a, i):
            width = grads[a].shape[-1] // self.pieces[a]
            if self.kinds[a] == "dz":
                return pl.ds(pl.multiple_of((me_t + n_t - 1 - i) % n_t * width, width), width)
            return pl.ds(i * width, width)

        def blocks(a, i, key, flipped=()):
            free, bit = cube.move(*key)
            rows = grads[a].shape[-2]
            span = cube.cuts(rows)[key[1]] if key[0] < cube.steps else pl.ds(0, rows)
            return grads[a].at[cube.index(free, flipped) + (span, columns(a, i))]

        def mine(a, i):
            return grads[a].at[cube.index(()) + (pl.ds(0, grads[a].shape[-2]), columns(a, i))]

        def landing(a, i, key):
            step, part = key
            if step == cube.steps:
                return core_in[a].at[i]
            return step_in[a][step].at[i, part]

        def d_copy(a, i, key):
            free, bit = cube.move(*key)
            return pltpu.make_async_remote_copy(
                src_ref=blocks(a, i, key, (bit,)),
                dst_ref=landing(a, i, key),
                send_sem=d_send.at[a, i, cube.row(key)],
                recv_sem=d_recv.at[a, i, cube.row(key)],
                device_id={"dp": cube.partner(bit)},
                device_id_type=MESH,
            )

        def add(a, i, key):
            free, bit = cube.move(*key)
            source = landing(a, i, key)
            rows = source.shape[-2]
            block = 16 if rows % 16 == 0 else 8
            first = cube.cuts(grads[a].shape[-2])[key[1]].start if key[0] < cube.steps else 0
            for number in range(1 << len(free)):
                held = sorted(free, reverse=True)
                bits = {b: number >> (len(held) - 1 - j) & 1 for j, b in enumerate(held)}
                target = grads[a].at[tuple(bits.get(b, cube.own(b)) for b in reversed(range(cube.bits)))]
                given = source.at[tuple(bits[b] for b in held)]

                def one(j, carry):
                    at = pl.ds(pl.multiple_of(j * block, block), block)
                    spot = (pl.ds(pl.multiple_of(first + j * block, block), block), columns(a, i))
                    target[spot] = (target[spot].astype(F32) + given[at, :].astype(F32)).astype(target.dtype)
                    return carry

                lax.fori_loop(0, rows // block, one, 0)

        def z_copy(a, i):
            other = (me_t + n_t - 1 - i) % n_t
            return pltpu.make_async_remote_copy(
                src_ref=mine(a, i if self.kinds[a] == "dz" else 0),
                dst_ref=z_in[a].at[me_t],
                send_sem=z_send.at[a, i],
                recv_sem=z_recv.at[a, me_t],
                device_id={"tensor": other},
                device_id_type=MESH,
            )

        def z_wait(a, r):
            other = (me_t + r) % n_t
            pltpu.make_async_remote_copy(
                src_ref=z_in[a].at[other],
                dst_ref=z_in[a].at[other],
                send_sem=z_send.at[a, 0],
                recv_sem=z_recv.at[a, other],
                device_id={"tensor": other},
                device_id_type=MESH,
            ).wait_recv()

        def advance(a, i, age):
            if age > 0:
                for key in cube.keys(cube.steps + 1 - age):
                    d_copy(a, i, key).wait_recv()
                    add(a, i, key)
            if age <= cube.steps:
                for key in cube.keys(cube.steps - age):
                    d_copy(a, i, key).start()
                return
            kind = self.kinds[a]
            if kind == "d":
                outs[a][:, columns(a, i)] = mine(a, i)[...].astype(F32)
            elif kind == "dz":
                if i < n_t - 1:
                    z_copy(a, i).start()
            else:
                for r in range(n_t - 1):
                    z_copy(a, r).start()

        most = max(self.pieces)
        order = range(count)
        for a in order:
            advance(a, 0, 0)
        for now in range(most + cube.steps + 1):
            for a in order:
                if now + 1 < self.pieces[a]:
                    advance(a, now + 1, 0)
            for age in range(cube.steps + 1, 0, -1):
                i = now + 1 - age
                for a in order:
                    if 0 <= i < self.pieces[a]:
                        advance(a, i, age)
        for a in order:
            if self.kinds[a] == "dz":
                for r in range(1, n_t):
                    z_wait(a, r)
                own = mine(a, n_t - 1)
                block = 16

                def total(j, carry, a=a, own=own):
                    at = pl.ds(pl.multiple_of(j * block, block), block)
                    value = own[at, :].astype(F32)
                    for r in range(1, n_t):
                        value = value + z_in[a][(me_t + r) % n_t, at, :].astype(F32)
                    outs[a][at, :] = value
                    return carry

                lax.fori_loop(0, own.shape[0] // block, total, 0)
            elif self.kinds[a] == "da":
                z_in[a][me_t] = mine(a, 0)[...]
                for r in range(1, n_t):
                    z_wait(a, r)
                value = z_in[a][0]
                for z in range(1, n_t):
                    value = value + z_in[a][z]
                outs[a][...] = value
        for a in order:
            for i in range(self.pieces[a]):
                for step in range(cube.steps + 1):
                    for key in cube.keys(step):
                        d_copy(a, i, key).wait_send()
            if self.kinds[a] != "d":
                for i in range(n_t - 1):
                    z_copy(a, i).wait_send()

    def __call__(self, *grads):
        count = len(grads)
        cube, n_t = self.cube, self.n_t
        outs, core, step, z = [], [], [], []
        for grad, kind, pieces in zip(grads, self.kinds, self.pieces):
            rows, cols = grad.shape[0] // cube.size, grad.shape[1] // pieces
            outs.append(jax.ShapeDtypeStruct((rows, cols if kind == "dz" else grad.shape[1]), F32))
            core.append(pltpu.VMEM((pieces,) + (2,) * cube.steps + (rows, cols), grad.dtype))
            for k in range(cube.steps):
                step.append(pltpu.VMEM((pieces, cube.parts) + (2,) * k + (rows // cube.parts, cols), grad.dtype))
            slots = (1, 8, 128) if kind == "d" else (n_t, rows, cols)
            z.append(pltpu.VMEM(slots, grad.dtype))
        most = max(self.pieces)
        keys = (cube.steps + 1) * cube.parts
        grads = [grad.reshape(cube.shape + (-1, grad.shape[1])) for grad in grads]
        return pl.pallas_call(
            self.kernel,
            out_shape=outs,
            in_specs=[pl.BlockSpec(memory_space=pltpu.VMEM)] * count,
            out_specs=[pl.BlockSpec(memory_space=pltpu.VMEM)] * count,
            scratch_shapes=core
            + z
            + step
            + [
                pltpu.SemaphoreType.DMA((count, most, keys)),
                pltpu.SemaphoreType.DMA((count, most, keys)),
                pltpu.SemaphoreType.DMA((count, n_t)),
                pltpu.SemaphoreType.DMA((count, n_t)),
            ],
            compiler_params=pltpu.CompilerParams(
                collective_id=self.ident, has_side_effects=True, vmem_limit_bytes=60 << 20
            ),
        )(*grads)


class Mlp:
    def __init__(self, n_t, ident):
        self.n_t, self.ident = n_t, ident

    def kernel(self, rows_ref, grad_ref, gu_hbm, down_hbm, all_ref, hid_ref, dgu_ref, back_ref, out_ref,
               gu, down, held, dy, dh, hid, dgu, back, out, own_sem, w_sem, dy_sem, put_sem, z_send, z_recv, b_send, b_recv):
        n_t = self.n_t
        me = lax.axis_index("tensor")
        units = down.shape[1]
        width = rows_ref.shape[1]
        interior = jnp.logical_and(me > 0, me < n_t - 1)

        barrier = pltpu.get_barrier_semaphore()
        for r in range(1, n_t):
            pl.semaphore_signal(barrier, inc=1, device_id={"tensor": (me + r) % n_t}, device_id_type=MESH)
        down_copy = pltpu.make_async_copy(down_hbm, down, w_sem.at[0])
        down_copy.start()
        gu_copy = pltpu.make_async_copy(gu_hbm, gu, w_sem.at[1])
        gu_copy.start()
        own_copy = pltpu.make_async_copy(rows_ref, held.at[me], own_sem)
        own_copy.start()

        def order(i):
            low, high = me, n_t - 1 - me
            both = 2 * jnp.minimum(low, high)
            near = i <= both
            distance = jnp.where(near, (i + 1) // 2, i - both // 2)
            way = jnp.where(near, (i + 1) % 2, jnp.where(low > high, 0, 1))
            return distance, way, jnp.where(way == 0, me - distance, me + distance)

        def piece_of(i):
            return order(i)[2]

        def hop(distance, way, piece, src=None):
            index = 2 * (distance - 1) + way
            return pltpu.make_async_remote_copy(
                src_ref=held.at[piece] if src is None else src,
                dst_ref=held.at[piece],
                send_sem=z_send.at[index],
                recv_sem=z_recv.at[index],
                device_id={"tensor": me + 1 - 2 * way},
                device_id_type=MESH,
            )

        def may_send(distance, way):
            room = jnp.where(way == 0, n_t - 1 - me, me)
            behind = jnp.where(way == 0, me, n_t - 1 - me)
            return jnp.logical_and(room > 0, behind >= distance - 1)

        def arrive(i):
            distance, way, piece = order(i)
            hop(distance, way, piece).wait_recv()

            @pl.when(may_send(distance + 1, way))
            def _():
                hop(distance + 1, way, piece).start()

        def dy_copy(i):
            return pltpu.make_async_copy(grad_ref.at[piece_of(i)], dy.at[i % 2], dy_sem.at[i % 2])

        def puts(i):
            piece, slot = piece_of(i), i % 2
            relative = (piece - me + n_t) % n_t
            return [
                pltpu.make_async_copy(hid.at[slot], hid_ref.at[piece], put_sem.at[slot, 0]),
                pltpu.make_async_copy(dgu.at[slot], dgu_ref.at[piece], put_sem.at[slot, 1]),
                pltpu.make_async_copy(out.at[slot], out_ref.at[relative], put_sem.at[slot, 2]),
            ]

        def keep(i):
            return pltpu.make_async_copy(held.at[piece_of(i)], all_ref.at[piece_of(i)], own_sem)

        def back_copy(i):
            piece = piece_of(i)
            return pltpu.make_async_remote_copy(
                src_ref=back.at[i],
                dst_ref=back_ref.at[me],
                send_sem=b_send.at[i],
                recv_sem=b_recv.at[me],
                device_id={"tensor": piece},
                device_id_type=MESH,
            )

        dy_copy(0).start()
        pl.semaphore_wait(barrier, n_t - 1)
        for way in (0, 1):

            @pl.when(may_send(1, way))
            def _():
                hop(1, way, me, rows_ref).start()

        own_copy.wait()
        down_copy.wait()
        wide = units // 256

        def chunk(i, carry):
            slot = i % 2
            piece = piece_of(i)

            @pl.when(jnp.logical_and(i > 0, jnp.logical_not(interior)))
            def _():
                arrive(i)

            @pl.when(jnp.logical_and(i == 1, interior))
            def _():
                arrive(i)

            @pl.when(jnp.logical_and(jnp.logical_and(i > 0, i + 1 < n_t), interior))
            def _():
                arrive(i + 1)

            @pl.when(i + 1 < n_t)
            def _():
                dy_copy(i + 1).start()

            @pl.when(i >= 2)
            def _():
                for put in puts(i - 2):
                    put.wait()

            dy_copy(i).wait()
            keep(i).start()

            def grad_tile(t, c):
                at = pl.ds(pl.multiple_of(t * 256, 256), 256)
                dh[:, at] = jnp.dot(dy[slot], down[:, at], preferred_element_type=F32)
                return c

            lax.fori_loop(0, wide, grad_tile, 0)
            if units % 256:
                dh[:, wide * 256 :] = jnp.dot(dy[slot], down[:, wide * 256 :], preferred_element_type=F32)

            @pl.when(i == 0)
            def _():
                gu_copy.wait()

            def unit_tile(t, c):
                at = pl.ds(pl.multiple_of(t * 128, 128), 128)
                pair = jnp.dot(held[piece], gu[:, pl.ds(pl.multiple_of(t * 256, 256), 256)], preferred_element_type=F32)
                gate, up = pair[:, :128], pair[:, 128:]
                sigmoid = jax.nn.sigmoid(gate)
                active = gate * sigmoid
                grad = dh[:, at]
                hid[slot, :, at] = (active * up).astype(BF16)
                first = grad * up * sigmoid * (1.0 + gate * (1.0 - sigmoid))
                dgu[slot, :, pl.ds(pl.multiple_of(t * 256, 128), 128)] = first.astype(BF16)
                dgu[slot, :, pl.ds(pl.multiple_of(t * 256 + 128, 128), 128)] = (grad * active).astype(BF16)
                return c

            lax.fori_loop(0, units // 128, unit_tile, 0)

            def back_tile(j, c):
                at = pl.ds(pl.multiple_of(j * 256, 256), 256)
                value = lax.dot_general(dgu[slot], gu[at, :], (((1,), (1,)), ((), ())), preferred_element_type=F32)
                back[i, :, at] = value.astype(BF16)
                return c

            lax.fori_loop(0, width // 256, back_tile, 0)

            @pl.when(i > 0)
            def _():
                back_copy(i).start()

            def out_tile(j, c):
                at = pl.ds(pl.multiple_of(j * 256, 256), 256)
                value = lax.dot_general(hid[slot], down[at, :], (((1,), (1,)), ((), ())), preferred_element_type=F32)
                out[slot, :, at] = value.astype(BF16)
                return c

            lax.fori_loop(0, width // 256, out_tile, 0)
            for put in puts(i):
                put.start()
            keep(i).wait()
            return carry

        lax.fori_loop(0, n_t, chunk, 0)
        mine = pltpu.make_async_copy(back.at[0], back_ref.at[me], own_sem)
        mine.start()
        for i in range(max(0, n_t - 2), n_t):
            for put in puts(i):
                put.wait()
        for r in range(1, n_t):
            other = (me + r) % n_t
            pltpu.make_async_remote_copy(
                src_ref=back_ref.at[other],
                dst_ref=back_ref.at[other],
                send_sem=b_send.at[0],
                recv_sem=b_recv.at[other],
                device_id={"tensor": other},
                device_id_type=MESH,
            ).wait_recv()
        mine.wait()
        for i in range(1, n_t):
            back_copy(i).wait_send()
        for k in range(1, n_t):
            for way in (0, 1):

                @pl.when(may_send(k, way))
                def _():
                    hop(k, way, me, rows_ref).wait_send()

    def __call__(self, rows, grads, w_gu, w_down):
        n_t = self.n_t
        tokens, width = rows.shape
        units = w_down.shape[1]
        hops = max(1, 2 * (n_t - 1))
        any_spec = pl.BlockSpec(memory_space=pl.ANY)

        def held(*shape):
            return pltpu.VMEM(shape, BF16)

        def put(cols):
            return jax.ShapeDtypeStruct((n_t, tokens, cols), BF16)

        return pl.pallas_call(
            self.kernel,
            out_shape=[put(width), put(units), put(2 * units), put(width), put(width)],
            in_specs=[pl.BlockSpec(memory_space=pltpu.VMEM), any_spec, any_spec, any_spec],
            out_specs=[any_spec] * 5,
            scratch_shapes=[
                held(width, 2 * units),
                held(width, units),
                held(n_t, tokens, width),
                held(2, tokens, width),
                pltpu.VMEM((tokens, units), F32),
                held(2, tokens, units),
                held(2, tokens, 2 * units),
                held(n_t, tokens, width),
                held(2, tokens, width),
                pltpu.SemaphoreType.DMA,
                pltpu.SemaphoreType.DMA((2,)),
                pltpu.SemaphoreType.DMA((2,)),
                pltpu.SemaphoreType.DMA((2, 3)),
                pltpu.SemaphoreType.DMA((hops,)),
                pltpu.SemaphoreType.DMA((hops,)),
                pltpu.SemaphoreType.DMA((n_t,)),
                pltpu.SemaphoreType.DMA((n_t,)),
            ],
            compiler_params=pltpu.CompilerParams(
                collective_id=self.ident, has_side_effects=True, vmem_limit_bytes=60 << 20
            ),
        )(rows, grads, w_gu, w_down)


def rope_tables(segments, start, rows):
    own = lax.dynamic_slice_in_dim(segments, start, rows, axis=1)
    earlier = jnp.sum((segments[:, None, :] < own[:, :, None]).astype(jnp.int32), axis=2)
    position = (start + jnp.arange(rows, dtype=jnp.int32)[None, :] - earlier).astype(F32)
    frequency = jnp.exp(jnp.arange(HD // 2, dtype=F32) * (-2.0 * math.log(10000.0) / HD))
    angles = position[..., None] * frequency
    return own, jnp.cos(angles), jnp.sin(angles)


def rotate(values, cosine, sine):
    half = values.shape[-1] // 2
    shape = cosine.shape[:2] + (1,) * (values.ndim - 3) + cosine.shape[2:]
    cosine, sine = cosine.reshape(shape), sine.reshape(shape)
    a, c = values[..., :half], values[..., half:]
    return jnp.concatenate([a * cosine - c * sine, c * cosine + a * sine], axis=-1)


def norm_forward(rows, gain):
    inv_rms = lax.rsqrt(jnp.mean(rows * rows, axis=-1, keepdims=True) + NORM_EPS)
    return (rows * inv_rms * gain).astype(BF16), inv_rms


def norm_backward(rows, inv_rms, gain, upstream):
    weighted = upstream * gain
    back = inv_rms * weighted - rows * (inv_rms * inv_rms * inv_rms) * jnp.mean(
        weighted * rows, axis=-1, keepdims=True
    )
    return back, jnp.sum(upstream * rows * inv_rms, axis=0)


def dot_nt(left, right):
    return lax.dot_general(left, right, (((1,), (1,)), ((), ())), preferred_element_type=F32)


def dot_tn(left, right):
    return lax.dot_general(left, right, (((0,), (0,)), ((), ())), preferred_element_type=F32)


def dot_nn(left, right):
    return jnp.dot(left, right, preferred_element_type=F32)


def dp_scatter(x):
    return lax.psum_scatter(x, "dp", scatter_dimension=0, tiled=True)


def body(
    heads, layer_input, segments, gain_attn, w_qkv, w_out_t, gain_mlp, w_gate_up, w_down_t, cotangent
):
    n_dp, n_t = lax.axis_size("dp"), lax.axis_size("tensor")
    me_t = lax.axis_index("tensor")
    batch, rows, width = layer_input.shape
    tokens = batch * rows
    shard_d = w_qkv.shape[0]
    groups = w_qkv.shape[1] * n_t
    q_cols = heads * HD
    parts = Cube(n_dp).parts

    x = layer_input.reshape(tokens, width)
    grad_in = cotangent.reshape(tokens, width)

    gu_w = w_gate_up.reshape(shard_d, 2, -1, 128).transpose(0, 2, 1, 3).reshape(shard_d, -1)
    gu_w = lax.all_gather(gu_w, "dp", axis=0, tiled=True)
    down_w = lax.all_gather(w_down_t, "dp", axis=0, tiled=True)
    w_local = w_qkv.reshape(shard_d, -1)
    gains = jnp.concatenate([gain_attn, gain_mlp]).astype(F32)
    gains = jnp.pad(gains, (0, 8 * parts * 128 - gains.shape[0])).reshape(8 * parts, 128)
    sources = [w_local[:, :q_cols], w_local[:, q_cols:], w_out_t, gains, grad_in.astype(BF16)]
    first = Gather(
        ["zd", "zd", "zd", "d", "z"], [0, 0, 0, 0, 1], [s.shape for s in sources], n_t, n_dp, 1
    )
    wq, wkv, wo, gains, grad_rows = first(*sources)
    gains = gains.reshape(n_dp, -1)[:, : 2 * shard_d].reshape(n_dp, 2, shard_d)
    g_attn = gains[:, 0].reshape(1, width)
    g_mlp = gains[:, 1].reshape(1, width)

    own_seg, cosine, sine = rope_tables(segments, me_t * rows, rows)
    normed_attn, scale_attn = norm_forward(x, g_attn)
    query = dot_nn(normed_attn, wq).reshape(batch, rows, groups, heads, HD)
    pairs = dot_nn(normed_attn, wkv).reshape(batch, rows, groups, 2 * HD)
    query = rotate(query, cosine, sine).astype(BF16)
    key = rotate(pairs[..., :HD], cosine, sine).astype(BF16)
    pairs = jnp.concatenate([key, pairs[..., HD:].astype(BF16)], axis=-1).reshape(tokens, -1)
    (pairs,) = Gather(["z"], [0], [pairs.shape], n_t, n_dp, 2)(pairs)
    pairs = pairs.reshape(n_t, batch, rows, groups, 2 * HD).transpose(1, 0, 2, 3, 4)
    pairs = pairs.reshape(batch, n_t * rows, groups, 2 * HD)
    keys, values = pairs[..., :HD], pairs[..., HD:]
    key_at = jnp.arange(n_t * rows, dtype=jnp.int32)
    own_at = me_t * rows + jnp.arange(rows, dtype=jnp.int32)
    allowed = (own_seg[:, :, None] == segments[:, None, :]) & (key_at[None, None, :] <= own_at[None, :, None])
    scores = jnp.einsum("bigne,bjge->bgnij", query, keys, preferred_element_type=F32) * (1.0 / math.sqrt(HD))
    scores = jnp.where(allowed[:, None, None], scores, F32(-1e30))
    row_max = jnp.max(scores, axis=-1, keepdims=True)
    log_total = row_max + jnp.log(jnp.sum(jnp.exp(scores - row_max), axis=-1, keepdims=True))
    weights = jnp.exp(scores - log_total)
    weights_b = weights.astype(BF16)
    mixed = jnp.einsum("bgnij,bjge->bigne", weights_b, values, preferred_element_type=F32)
    mixed = mixed.astype(BF16).reshape(tokens, -1)
    residual = x + dot_nt(mixed, wo)

    normed_mlp, scale_mlp = norm_forward(residual, g_mlp)
    mlp_rows, hidden, grad_gu, back_parts, out_parts = Mlp(n_t, 3)(normed_mlp, grad_rows, gu_w, down_w)
    total = residual + out_parts[0].astype(F32)
    for r in range(1, n_t):
        total = total + lax.ppermute(out_parts[r], "tensor", [(i, (i + r) % n_t) for i in range(n_t)]).astype(F32)
    output = total
    flat = n_t * tokens
    down_grad = dp_scatter(dot_tn(grad_rows.reshape(flat, width), hidden.reshape(flat, -1)).astype(BF16)).astype(F32)
    gate_up_grad = dp_scatter(dot_tn(mlp_rows.reshape(flat, width), grad_gu.reshape(flat, -1)).astype(BF16))
    gate_up_grad = gate_up_grad.astype(F32).reshape(shard_d, -1, 2, 128).transpose(0, 2, 1, 3)

    grad_normed = jnp.sum(back_parts.astype(F32), axis=0)
    back_mlp, gain_mlp_part = norm_backward(residual, scale_mlp, g_mlp, grad_normed)
    grad_resid = grad_in + back_mlp
    resid_b = grad_resid.astype(BF16)

    out_grad = dot_tn(resid_b, mixed).astype(BF16)
    grad_mixed = dot_nn(resid_b, wo).astype(BF16).reshape(batch, rows, groups, heads, HD)
    grad_value = jnp.einsum("bgnij,bigne->bjge", weights_b, grad_mixed, preferred_element_type=F32)
    grad_weights = jnp.einsum("bigne,bjge->bgnij", grad_mixed, values, preferred_element_type=F32)
    grad_scores = (
        weights
        * (grad_weights - jnp.sum(weights * grad_weights, axis=-1, keepdims=True))
        * (1.0 / math.sqrt(HD))
    ).astype(BF16)
    grad_query = jnp.einsum("bgnij,bjge->bigne", grad_scores, keys, preferred_element_type=F32)
    grad_key = jnp.einsum("bgnij,bigne->bjge", grad_scores, query, preferred_element_type=F32)
    grad_pairs = jnp.concatenate([grad_key, grad_value], axis=-1).astype(BF16)
    grad_pairs = lax.psum_scatter(grad_pairs, "tensor", scatter_dimension=1, tiled=True).astype(F32)
    grad_query = rotate(grad_query, cosine, -sine).astype(BF16).reshape(tokens, -1)
    grad_key = rotate(grad_pairs[..., :HD], cosine, -sine)
    grad_pairs = jnp.concatenate([grad_key, grad_pairs[..., HD:]], axis=-1).astype(BF16).reshape(tokens, -1)
    q_grad = dot_tn(normed_attn, grad_query).astype(BF16)
    kv_grad = dot_tn(normed_attn, grad_pairs).astype(BF16)
    grad_normed_attn = dot_nt(grad_query, wq) + dot_nt(grad_pairs, wkv)
    back_attn, gain_attn_part = norm_backward(x, scale_attn, g_attn, grad_normed_attn)
    input_grad = grad_resid + back_attn

    gain_parts = jnp.stack([gain_attn_part.reshape(n_dp, -1), gain_mlp_part.reshape(n_dp, -1)], axis=1)
    gain_parts = gain_parts.reshape(n_dp, -1)
    gain_parts = jnp.pad(gain_parts, ((0, 0), (0, 8 * parts * 128 - gain_parts.shape[1]))).reshape(-1, 128)
    q_grad, kv_grad, out_grad, gain_grads = Scatter(["dz", "dz", "dz", "da"], [1, 1, 1, 1], n_t, n_dp, 4)(
        q_grad, kv_grad, out_grad, gain_parts
    )
    qkv_grad = jnp.concatenate([q_grad, kv_grad], axis=1)
    gain_grads = gain_grads.reshape(-1)[: 2 * shard_d]
    gain_first, gain_second = gain_grads[:shard_d], gain_grads[shard_d:]
    return (
        output.reshape(layer_input.shape),
        input_grad.reshape(layer_input.shape),
        gain_first,
        qkv_grad.reshape(w_qkv.shape),
        out_grad,
        gain_second,
        gate_up_grad.reshape(w_gate_up.shape),
        down_grad,
    )


def solution(mesh):
    placed = (
        P("dp", "tensor", None),
        P("dp", None),
        P("dp"),
        P("dp", "tensor", None),
        P("dp", "tensor"),
        P("dp"),
        P("dp", None, "tensor"),
        P("dp", "tensor"),
        P("dp", "tensor", None),
    )

    def whole(*args):
        heads = args[3].shape[2] // HD - 2
        return jax.shard_map(
            functools.partial(body, heads),
            mesh=mesh,
            in_specs=placed,
            out_specs=(placed[0], placed[0], P("dp"), placed[3], placed[4], P("dp"), placed[6], placed[7]),
            check_vma=False,
        )(*args)

    return whole
```

```python
import functools
import math

import jax
import jax.numpy as jnp
from jax import lax
from jax.experimental import pallas as pl
from jax.experimental.pallas import tpu as pltpu
from jax.sharding import PartitionSpec as P

HD = 64
NORM_EPS = 1e-05
F32 = jnp.float32
BF16 = jnp.bfloat16
MESH = pl.DeviceIdType.MESH
LATE = 2


class Cube:
    def __init__(self, size):
        self.size = size
        self.bits = size.bit_length() - 1
        assert 1 << self.bits == size and self.bits >= 1
        self.shape = (2,) * self.bits
        outer = list(range(1, self.bits))
        self.steps = len(outer)
        self.parts = max(1, self.steps)
        self.orders = [outer[p:] + outer[:p] for p in range(self.parts)]

    def own(self, bit):
        return lax.axis_index("dp") // (1 << bit) % 2

    def partner(self, bit):
        return lax.axis_index("dp") + (1 << bit) * (1 - 2 * self.own(bit))

    def index(self, free, flipped=()):
        spots = []
        for bit in reversed(range(self.bits)):
            if bit in free:
                spots.append(slice(None))
            else:
                spots.append(1 - self.own(bit) if bit in flipped else self.own(bit))
        return tuple(spots)

    def cuts(self, rows):
        count = rows // self.parts
        return [pl.ds(part * count, count) for part in range(self.parts)]

    def move(self, step, part):
        if step == self.steps:
            return tuple(range(1, self.bits)), 0
        return tuple(self.orders[part][:step]), self.orders[part][step]

    def keys(self, step):
        return [(step, part) for part in range(self.parts if step < self.steps else 1)]

    def row(self, key):
        return key[0] * self.parts + key[1]


class Gather:
    def __init__(self, kinds, late, shapes, n_t, n_dp, ident):
        self.kinds, self.late, self.shapes = kinds, late, shapes
        self.n_t, self.cube, self.ident = n_t, Cube(n_dp), ident
        self.ticks = [[("own", 0)]] + [[("up", k), ("down", k)] for k in range(1, n_t)]
        self.insts = [inst for tick in self.ticks for inst in tick]
        self.uses_dp = any("d" in kind for kind in kinds)
        self.uses_z = any("z" in kind for kind in kinds)
    def out_shape(self, a):
        rows, cols = self.shapes[a]
        kind = self.kinds[a]
        if kind == "z":
            return (self.n_t, rows, cols)
        return self.cube.shape + (rows, cols * (self.n_t if "z" in kind else 1))

    def place(self, ref, a, z, free=(), flipped=(), part=None):
        rows, cols = self.shapes[a]
        kind = self.kinds[a]
        if kind == "z":
            return ref.at[z]
        span = pl.ds(0, rows) if part is None else self.cube.cuts(rows)[part]
        width = pl.ds(pl.multiple_of(z * cols, cols), cols) if "z" in kind else pl.ds(0, cols)
        return ref.at[self.cube.index(free, flipped) + (span, width)]

    def kernel(self, *refs):
        count = len(self.kinds)
        srcs, dests = refs[:count], refs[count : 2 * count]
        own_sem, z_send, z_recv, d_send, d_recv = refs[2 * count :]
        n_t, cube = self.n_t, self.cube
        me_t = lax.axis_index("tensor")
        main = [a for a in range(count) if not self.late[a]]
        tail = [a for a in range(count) if self.late[a]]

        barrier = pltpu.get_barrier_semaphore()
        if self.uses_dp:
            for bit in range(cube.bits):
                pl.semaphore_signal(barrier, inc=1, device_id={"dp": cube.partner(bit)}, device_id_type=MESH)
        peers = self.n_t - 1 if self.uses_z else 0
        for r in range(peers):
            pl.semaphore_signal(barrier, inc=1, device_id={"tensor": (me_t + 1 + r) % n_t}, device_id_type=MESH)
        pl.semaphore_wait(barrier, peers + (cube.bits if self.uses_dp else 0))

        def own_copy(a):
            return pltpu.make_async_copy(srcs[a], self.place(dests[a], a, me_t), own_sem.at[a])

        for a in range(count):
            own_copy(a).start()

        def piece_of(inst):
            way, k = inst
            return me_t if way == "own" else me_t - k if way == "up" else me_t + k

        def exists(inst, fn):
            way, k = inst
            if way == "own":
                fn()
            elif way == "up":
                pl.when(me_t >= k)(fn)
            else:
                pl.when(me_t + k < n_t)(fn)

        def z_copy(a, way, k, src):
            piece = me_t - (k - 1) if way == "up" else me_t + (k - 1)
            index = 2 * (k - 1) + (way == "down")
            dest = self.place(dests[a], a, piece)
            return pltpu.make_async_remote_copy(
                src_ref=dest if src is None else src,
                dst_ref=dest,
                send_sem=z_send.at[a, index],
                recv_sem=z_recv.at[a, index],
                device_id={"tensor": me_t + 1 if way == "up" else me_t - 1},
                device_id_type=MESH,
            )

        def z_cond(way, k):
            return (
                jnp.logical_and(me_t >= k - 1, me_t < n_t - 1)
                if way == "up"
                else jnp.logical_and(me_t + (k - 1) < n_t, me_t > 0)
            )

        def z_start(a, inst):
            way, k = inst
            for out_way in ("up", "down") if way == "own" else (way,):
                if k + 1 < n_t:

                    @pl.when(z_cond(out_way, k + 1))
                    def _():
                        z_copy(a, out_way, k + 1, srcs[a] if way == "own" else None).start()

        def z_arrive(a, inst):
            way, k = inst
            if way != "own":
                index = 2 * (k - 1) + (way == "down")
                dest = self.place(dests[a], a, piece_of(inst))
                pltpu.make_async_remote_copy(
                    src_ref=dest,
                    dst_ref=dest,
                    send_sem=z_send.at[a, index],
                    recv_sem=z_recv.at[a, index],
                    device_id={"tensor": me_t},
                    device_id_type=MESH,
                ).wait_recv()

        def d_copy(a, inst, key, incoming=False):
            free, bit = cube.move(*key)
            part = key[1] if key[0] < cube.steps else None
            spot = self.place(dests[a], a, piece_of(inst), free, (bit,) if incoming else (), part)
            sem = (a, self.insts.index(inst), cube.row(key))
            return pltpu.make_async_remote_copy(
                src_ref=spot,
                dst_ref=spot,
                send_sem=d_send.at[sem],
                recv_sem=d_recv.at[sem],
                device_id={"dp": cube.partner(bit)},
                device_id_type=MESH,
            )

        def d_advance(a, inst, stage):
            if stage == 0 and inst[0] == "own":
                own_copy(a).wait()
            if stage > 0:
                for key in cube.keys(stage - 1):
                    d_copy(a, inst, key, True).wait_recv()
            if stage <= cube.steps:
                for key in cube.keys(stage):
                    d_copy(a, inst, key).start()

        def in_dp(a, inst):
            return "d" in self.kinds[a] and (inst[0] == "own" or "z" in self.kinds[a])

        z_main = [a for a in main if "z" in self.kinds[a]]
        z_tail = [a for a in tail if "z" in self.kinds[a]]
        length = n_t if self.uses_z else 1
        total = max(length + cube.steps + 2, 2 * length + 1)
        for now in range(total):
            for inst in self.ticks[now] if now < length else ():
                def arrive(inst=inst):
                    for a in z_main:
                        z_arrive(a, inst)
                        z_start(a, inst)
                    for a in main:
                        if in_dp(a, inst):
                            d_advance(a, inst, 0)

                exists(inst, arrive)
            late_now = now - length + LATE
            if 0 <= late_now < length and z_tail:
                for inst in self.ticks[late_now]:
                    def arrive_late(inst=inst):
                        for a in z_tail:
                            z_arrive(a, inst)
                            z_start(a, inst)

                    exists(inst, arrive_late)
            for age in range(1, cube.steps + 2):
                tick = now - age
                for inst in self.ticks[tick] if 0 <= tick < length else ():
                    def advance(inst=inst, age=age):
                        for a in main:
                            if in_dp(a, inst):
                                d_advance(a, inst, age)

                    exists(inst, advance)

        for inst in self.insts:
            def drain(inst=inst):
                for a in main:
                    if in_dp(a, inst):
                        for stage in range(cube.steps + 1):
                            for key in cube.keys(stage):
                                d_copy(a, inst, key).wait_send()

            exists(inst, drain)
        for a in range(count):
            if "z" in self.kinds[a]:
                for k in range(1, n_t):
                    for way in ("up", "down"):

                        @pl.when(z_cond(way, k))
                        def _():
                            z_copy(a, way, k, srcs[a] if k == 1 else None).wait_send()

            if not in_dp(a, ("own", 0)):
                own_copy(a).wait()

    def __call__(self, *arrays):
        count = len(arrays)
        n_z = max(1, 2 * (self.n_t - 1))
        rows = (self.cube.steps + 1) * self.cube.parts
        insts = len(self.insts) if self.uses_dp else 1
        outs = pl.pallas_call(
            self.kernel,
            out_shape=[jax.ShapeDtypeStruct(self.out_shape(a), arrays[a].dtype) for a in range(count)],
            in_specs=[pl.BlockSpec(memory_space=pltpu.VMEM)] * count,
            out_specs=[pl.BlockSpec(memory_space=pl.ANY)] * count,
            scratch_shapes=[
                pltpu.SemaphoreType.DMA((count,)),
                pltpu.SemaphoreType.DMA((count, n_z)),
                pltpu.SemaphoreType.DMA((count, n_z)),
                pltpu.SemaphoreType.DMA((count, insts, rows)),
                pltpu.SemaphoreType.DMA((count, insts, rows)),
            ],
            compiler_params=pltpu.CompilerParams(collective_id=self.ident, has_side_effects=True),
        )(*arrays)
        return [
            out.reshape(-1, out.shape[-1]) if "d" in kind else out for out, kind in zip(outs, self.kinds)
        ]


class Scatter:
    def __init__(self, kinds, pieces, n_t, n_dp, ident):
        self.kinds = kinds
        self.pieces = [n_t if kind == "dz" else count for kind, count in zip(kinds, pieces)]
        self.n_t, self.cube, self.ident = n_t, Cube(n_dp), ident

    def kernel(self, *refs):
        count = len(self.kinds)
        n_t, cube = self.n_t, self.cube
        grads, outs = refs[:count], refs[count : 2 * count]
        core_in, z_in = refs[2 * count : 3 * count], refs[3 * count : 4 * count]
        step_in = [refs[4 * count + a * cube.steps :][: cube.steps] for a in range(count)]
        d_send, d_recv, z_send, z_recv = refs[-4:]
        me_t = lax.axis_index("tensor")
        to_z = any(kind != "d" for kind in self.kinds)

        barrier = pltpu.get_barrier_semaphore()
        for bit in range(cube.bits):
            pl.semaphore_signal(barrier, inc=1, device_id={"dp": cube.partner(bit)}, device_id_type=MESH)
        if to_z:
            for r in range(1, n_t):
                pl.semaphore_signal(barrier, inc=1, device_id={"tensor": (me_t + r) % n_t}, device_id_type=MESH)
        pl.semaphore_wait(barrier, cube.bits + (n_t - 1 if to_z else 0))

        def columns(a, i):
            width = grads[a].shape[-1] // self.pieces[a]
            if self.kinds[a] == "dz":
                return pl.ds(pl.multiple_of((me_t + n_t - 1 - i) % n_t * width, width), width)
            return pl.ds(i * width, width)

        def blocks(a, i, key, flipped=()):
            free, bit = cube.move(*key)
            rows = grads[a].shape[-2]
            span = cube.cuts(rows)[key[1]] if key[0] < cube.steps else pl.ds(0, rows)
            return grads[a].at[cube.index(free, flipped) + (span, columns(a, i))]

        def mine(a, i):
            return grads[a].at[cube.index(()) + (pl.ds(0, grads[a].shape[-2]), columns(a, i))]

        def landing(a, i, key):
            step, part = key
            if step == cube.steps:
                return core_in[a].at[i]
            return step_in[a][step].at[i, part]

        def d_copy(a, i, key):
            free, bit = cube.move(*key)
            return pltpu.make_async_remote_copy(
                src_ref=blocks(a, i, key, (bit,)),
                dst_ref=landing(a, i, key),
                send_sem=d_send.at[a, i, cube.row(key)],
                recv_sem=d_recv.at[a, i, cube.row(key)],
                device_id={"dp": cube.partner(bit)},
                device_id_type=MESH,
            )

        def add(a, i, key):
            free, bit = cube.move(*key)
            source = landing(a, i, key)
            rows = source.shape[-2]
            block = 16 if rows % 16 == 0 else 8
            first = cube.cuts(grads[a].shape[-2])[key[1]].start if key[0] < cube.steps else 0
            for number in range(1 << len(free)):
                held = sorted(free, reverse=True)
                bits = {b: number >> (len(held) - 1 - j) & 1 for j, b in enumerate(held)}
                target = grads[a].at[tuple(bits.get(b, cube.own(b)) for b in reversed(range(cube.bits)))]
                given = source.at[tuple(bits[b] for b in held)]

                def one(j, carry):
                    at = pl.ds(pl.multiple_of(j * block, block), block)
                    spot = (pl.ds(pl.multiple_of(first + j * block, block), block), columns(a, i))
                    target[spot] = (target[spot].astype(F32) + given[at, :].astype(F32)).astype(target.dtype)
                    return carry

                lax.fori_loop(0, rows // block, one, 0)

        def z_copy(a, i):
            other = (me_t + n_t - 1 - i) % n_t
            return pltpu.make_async_remote_copy(
                src_ref=mine(a, i if self.kinds[a] == "dz" else 0),
                dst_ref=z_in[a].at[me_t],
                send_sem=z_send.at[a, i],
                recv_sem=z_recv.at[a, me_t],
                device_id={"tensor": other},
                device_id_type=MESH,
            )

        def z_wait(a, r):
            other = (me_t + r) % n_t
            pltpu.make_async_remote_copy(
                src_ref=z_in[a].at[other],
                dst_ref=z_in[a].at[other],
                send_sem=z_send.at[a, 0],
                recv_sem=z_recv.at[a, other],
                device_id={"tensor": other},
                device_id_type=MESH,
            ).wait_recv()

        def advance(a, i, age):
            if age > 0:
                for key in cube.keys(cube.steps + 1 - age):
                    d_copy(a, i, key).wait_recv()
                    add(a, i, key)
            if age <= cube.steps:
                for key in cube.keys(cube.steps - age):
                    d_copy(a, i, key).start()
                return
            kind = self.kinds[a]
            if kind == "d":
                outs[a][:, columns(a, i)] = mine(a, i)[...].astype(F32)
            elif kind == "dz":
                if i < n_t - 1:
                    z_copy(a, i).start()
            else:
                for r in range(n_t - 1):
                    z_copy(a, r).start()

        most = max(self.pieces)
        order = range(count)
        for a in order:
            advance(a, 0, 0)
        for now in range(most + cube.steps + 1):
            for a in order:
                if now + 1 < self.pieces[a]:
                    advance(a, now + 1, 0)
            for age in range(cube.steps + 1, 0, -1):
                i = now + 1 - age
                for a in order:
                    if 0 <= i < self.pieces[a]:
                        advance(a, i, age)
        for a in order:
            if self.kinds[a] == "dz":
                for r in range(1, n_t):
                    z_wait(a, r)
                own = mine(a, n_t - 1)
                block = 16

                def total(j, carry, a=a, own=own):
                    at = pl.ds(pl.multiple_of(j * block, block), block)
                    value = own[at, :].astype(F32)
                    for r in range(1, n_t):
                        value = value + z_in[a][(me_t + r) % n_t, at, :].astype(F32)
                    outs[a][at, :] = value
                    return carry

                lax.fori_loop(0, own.shape[0] // block, total, 0)
            elif self.kinds[a] == "da":
                z_in[a][me_t] = mine(a, 0)[...]
                for r in range(1, n_t):
                    z_wait(a, r)
                value = z_in[a][0]
                for z in range(1, n_t):
                    value = value + z_in[a][z]
                outs[a][...] = value
        for a in order:
            for i in range(self.pieces[a]):
                for step in range(cube.steps + 1):
                    for key in cube.keys(step):
                        d_copy(a, i, key).wait_send()
            if self.kinds[a] != "d":
                for i in range(n_t - 1):
                    z_copy(a, i).wait_send()

    def __call__(self, *grads):
        count = len(grads)
        cube, n_t = self.cube, self.n_t
        outs, core, step, z = [], [], [], []
        for grad, kind, pieces in zip(grads, self.kinds, self.pieces):
            rows, cols = grad.shape[0] // cube.size, grad.shape[1] // pieces
            outs.append(jax.ShapeDtypeStruct((rows, cols if kind == "dz" else grad.shape[1]), F32))
            core.append(pltpu.VMEM((pieces,) + (2,) * cube.steps + (rows, cols), grad.dtype))
            for k in range(cube.steps):
                step.append(pltpu.VMEM((pieces, cube.parts) + (2,) * k + (rows // cube.parts, cols), grad.dtype))
            slots = (1, 8, 128) if kind == "d" else (n_t, rows, cols)
            z.append(pltpu.VMEM(slots, grad.dtype))
        most = max(self.pieces)
        keys = (cube.steps + 1) * cube.parts
        grads = [grad.reshape(cube.shape + (-1, grad.shape[1])) for grad in grads]
        return pl.pallas_call(
            self.kernel,
            out_shape=outs,
            in_specs=[pl.BlockSpec(memory_space=pltpu.VMEM)] * count,
            out_specs=[pl.BlockSpec(memory_space=pltpu.VMEM)] * count,
            scratch_shapes=core
            + z
            + step
            + [
                pltpu.SemaphoreType.DMA((count, most, keys)),
                pltpu.SemaphoreType.DMA((count, most, keys)),
                pltpu.SemaphoreType.DMA((count, n_t)),
                pltpu.SemaphoreType.DMA((count, n_t)),
            ],
            compiler_params=pltpu.CompilerParams(
                collective_id=self.ident, has_side_effects=True, vmem_limit_bytes=60 << 20
            ),
        )(*grads)


class Mlp:
    def __init__(self, n_t, ident):
        self.n_t, self.ident = n_t, ident

    def kernel(self, rows_ref, grad_ref, w_hbm, all_ref, hid_ref, dgu_ref, back_ref, *refs):
        out_refs = refs[: self.n_t]
        (gu, down, held, dy, dh, hid, dgu, flat, back, out, own_sem, w_sem, dy_sem, put_sem, z_send, z_recv, b_send, b_recv) = refs[self.n_t :]
        n_t = self.n_t
        me = lax.axis_index("tensor")
        units = down.shape[1]
        width = rows_ref.shape[1]
        interior = jnp.logical_and(me > 0, me < n_t - 1)

        barrier = pltpu.get_barrier_semaphore()
        for r in range(1, n_t):
            pl.semaphore_signal(barrier, inc=1, device_id={"tensor": (me + r) % n_t}, device_id_type=MESH)
        down_copy = pltpu.make_async_copy(w_hbm.at[:, pl.ds(2 * units, units)], down, w_sem.at[0])
        down_copy.start()
        gu_copy = pltpu.make_async_copy(w_hbm.at[:, pl.ds(0, 2 * units)], gu, w_sem.at[1])
        gu_copy.start()
        own_copy = pltpu.make_async_copy(rows_ref, held.at[me], own_sem)
        own_copy.start()

        def order(i):
            low, high = me, n_t - 1 - me
            both = 2 * jnp.minimum(low, high)
            near = i <= both
            distance = jnp.where(near, (i + 1) // 2, i - both // 2)
            way = jnp.where(near, (i + 1) % 2, jnp.where(low > high, 0, 1))
            return distance, way, jnp.where(way == 0, me - distance, me + distance)

        def piece_of(i):
            return order(i)[2]

        def hop(distance, way, piece, src=None):
            index = 2 * (distance - 1) + way
            return pltpu.make_async_remote_copy(
                src_ref=held.at[piece] if src is None else src,
                dst_ref=held.at[piece],
                send_sem=z_send.at[index],
                recv_sem=z_recv.at[index],
                device_id={"tensor": me + 1 - 2 * way},
                device_id_type=MESH,
            )

        def may_send(distance, way):
            room = jnp.where(way == 0, n_t - 1 - me, me)
            behind = jnp.where(way == 0, me, n_t - 1 - me)
            return jnp.logical_and(room > 0, behind >= distance - 1)

        def arrive(i):
            distance, way, piece = order(i)
            hop(distance, way, piece).wait_recv()

            @pl.when(may_send(distance + 1, way))
            def _():
                hop(distance + 1, way, piece).start()

        def dy_copy(i):
            return pltpu.make_async_copy(grad_ref.at[piece_of(i)], dy.at[i % 2], dy_sem.at[i % 2])

        def puts(i):
            piece, slot = piece_of(i), i % 2
            return [
                pltpu.make_async_copy(hid.at[slot], hid_ref.at[piece], put_sem.at[slot, 0]),
                pltpu.make_async_copy(flat.at[slot], dgu_ref.at[piece], put_sem.at[slot, 1]),
            ]

        def out_put(i, r=0):
            return pltpu.make_async_copy(out.at[i % 2], out_refs[r], put_sem.at[i % 2, 2])

        def put_start(i):
            for put in puts(i):
                put.start()
            for r in range(n_t):

                @pl.when((piece_of(i) - me + n_t) % n_t == r)
                def _():
                    out_put(i, r).start()

        def put_wait(i):
            for put in puts(i):
                put.wait()
            out_put(i).wait()

        def keep(i):
            return pltpu.make_async_copy(held.at[piece_of(i)], all_ref.at[piece_of(i)], own_sem)

        def back_copy(i):
            piece = piece_of(i)
            return pltpu.make_async_remote_copy(
                src_ref=back.at[i],
                dst_ref=back_ref.at[me],
                send_sem=b_send.at[i],
                recv_sem=b_recv.at[me],
                device_id={"tensor": piece},
                device_id_type=MESH,
            )

        dy_copy(0).start()
        pl.semaphore_wait(barrier, n_t - 1)
        for way in (0, 1):

            @pl.when(may_send(1, way))
            def _():
                hop(1, way, me, rows_ref).start()

        own_copy.wait()
        down_copy.wait()
        wide = units // 256

        def chunk(i, carry):
            slot = i % 2
            piece = piece_of(i)

            @pl.when(jnp.logical_and(i > 0, jnp.logical_not(interior)))
            def _():
                arrive(i)

            @pl.when(jnp.logical_and(i == 1, interior))
            def _():
                arrive(i)

            @pl.when(jnp.logical_and(jnp.logical_and(i > 0, i + 1 < n_t), interior))
            def _():
                arrive(i + 1)

            @pl.when(i + 1 < n_t)
            def _():
                dy_copy(i + 1).start()

            @pl.when(i >= 2)
            def _():
                put_wait(i - 2)

            dy_copy(i).wait()
            keep(i).start()

            def grad_tile(t, c):
                at = pl.ds(pl.multiple_of(t * 256, 256), 256)
                dh[:, at] = jnp.dot(dy[slot], down[:, at], preferred_element_type=F32)
                return c

            lax.fori_loop(0, wide, grad_tile, 0)
            if units % 256:
                dh[:, wide * 256 :] = jnp.dot(dy[slot], down[:, wide * 256 :], preferred_element_type=F32)

            @pl.when(i == 0)
            def _():
                gu_copy.wait()

            def unit_tile(t, c):
                at = pl.ds(pl.multiple_of(t * 128, 128), 128)
                pair = jnp.dot(held[piece], gu[:, pl.ds(pl.multiple_of(t * 256, 256), 256)], preferred_element_type=F32)
                gate, up = pair[:, :128], pair[:, 128:]
                sigmoid = jax.nn.sigmoid(gate)
                active = gate * sigmoid
                grad = dh[:, at]
                hid[slot, :, at] = (active * up).astype(BF16)
                first = (grad * up * sigmoid * (1.0 + gate * (1.0 - sigmoid))).astype(BF16)
                second = (grad * active).astype(BF16)
                dgu[slot, :, pl.ds(pl.multiple_of(t * 256, 128), 128)] = first
                dgu[slot, :, pl.ds(pl.multiple_of(t * 256 + 128, 128), 128)] = second
                flat[slot, :, at] = first
                flat[slot, :, pl.ds(pl.multiple_of(units + t * 128, 128), 128)] = second
                return c

            lax.fori_loop(0, units // 128, unit_tile, 0)

            def back_tile(j, c):
                at = pl.ds(pl.multiple_of(j * 256, 256), 256)
                value = lax.dot_general(dgu[slot], gu[at, :], (((1,), (1,)), ((), ())), preferred_element_type=F32)
                back[i, :, at] = value.astype(BF16)
                return c

            lax.fori_loop(0, width // 256, back_tile, 0)

            @pl.when(i > 0)
            def _():
                back_copy(i).start()

            def out_tile(j, c):
                at = pl.ds(pl.multiple_of(j * 256, 256), 256)
                value = lax.dot_general(hid[slot], down[at, :], (((1,), (1,)), ((), ())), preferred_element_type=F32)
                out[slot, :, at] = value.astype(BF16)
                return c

            lax.fori_loop(0, width // 256, out_tile, 0)
            put_start(i)
            keep(i).wait()
            return carry

        lax.fori_loop(0, n_t, chunk, 0)
        mine = pltpu.make_async_copy(back.at[0], back_ref.at[me], own_sem)
        mine.start()
        for i in range(max(0, n_t - 2), n_t):
            put_wait(i)
        for r in range(1, n_t):
            other = (me + r) % n_t
            pltpu.make_async_remote_copy(
                src_ref=back_ref.at[other],
                dst_ref=back_ref.at[other],
                send_sem=b_send.at[0],
                recv_sem=b_recv.at[other],
                device_id={"tensor": other},
                device_id_type=MESH,
            ).wait_recv()
        mine.wait()
        for i in range(1, n_t):
            back_copy(i).wait_send()
        for k in range(1, n_t):
            for way in (0, 1):

                @pl.when(may_send(k, way))
                def _():
                    hop(k, way, me, rows_ref).wait_send()

    def __call__(self, rows, grads, weights):
        n_t = self.n_t
        tokens, width = rows.shape
        units = weights.shape[1] // 3
        hops = max(1, 2 * (n_t - 1))
        any_spec = pl.BlockSpec(memory_space=pl.ANY)

        def held(*shape):
            return pltpu.VMEM(shape, BF16)

        def put(cols, *lead):
            return jax.ShapeDtypeStruct(lead + (tokens, cols), BF16)

        return pl.pallas_call(
            self.kernel,
            out_shape=[put(width, n_t), put(units, n_t), put(2 * units, n_t), put(width, n_t)] + [put(width)] * n_t,
            in_specs=[pl.BlockSpec(memory_space=pltpu.VMEM), any_spec, any_spec],
            out_specs=[any_spec] * (4 + n_t),
            scratch_shapes=[
                held(width, 2 * units),
                held(width, units),
                held(n_t, tokens, width),
                held(2, tokens, width),
                pltpu.VMEM((tokens, units), F32),
                held(2, tokens, units),
                held(2, tokens, 2 * units),
                held(2, tokens, 2 * units),
                held(n_t, tokens, width),
                held(2, tokens, width),
                pltpu.SemaphoreType.DMA,
                pltpu.SemaphoreType.DMA((2,)),
                pltpu.SemaphoreType.DMA((2,)),
                pltpu.SemaphoreType.DMA((2, 3)),
                pltpu.SemaphoreType.DMA((hops,)),
                pltpu.SemaphoreType.DMA((hops,)),
                pltpu.SemaphoreType.DMA((n_t,)),
                pltpu.SemaphoreType.DMA((n_t,)),
            ],
            compiler_params=pltpu.CompilerParams(
                collective_id=self.ident, has_side_effects=True, vmem_limit_bytes=60 << 20
            ),
        )(rows, grads, weights)


def turn(x, table, sign):
    cosine, low, high = table[:, :128], table[:, 128:256], table[:, 256:]
    return x * cosine + sign * (pltpu.roll(x, 96, 1) * low + pltpu.roll(x, 32, 1) * high)


def rope_kernel(q_ref, kv_ref, table_ref, qo_ref, kvo_ref):
    table, pair_table = table_ref[:, :384], table_ref[:, 384:]
    for j in range(q_ref.shape[1] // 128):
        at = slice(128 * j, 128 * j + 128)
        qo_ref[:, at] = turn(q_ref[:, at], table, 1.0).astype(BF16)
    for j in range(kv_ref.shape[1] // 128):
        at = slice(128 * j, 128 * j + 128)
        kvo_ref[:, at] = turn(kv_ref[:, at], pair_table, 1.0).astype(BF16)


def rope(q, kv, table):
    rows = q.shape[0]
    block = math.gcd(rows, 64)

    def spec(x):
        return pl.BlockSpec((block, x.shape[1]), lambda i: (i, 0))

    return pl.pallas_call(
        rope_kernel,
        grid=(rows // block,),
        out_shape=[jax.ShapeDtypeStruct(q.shape, BF16), jax.ShapeDtypeStruct(kv.shape, BF16)],
        in_specs=[spec(q), spec(kv), spec(table)],
        out_specs=[spec(q), spec(kv)],
    )(q, kv, table)


def stacked(x):
    return jnp.concatenate([x[:, HD * h : HD * (h + 1)] for h in range(x.shape[1] // HD)], axis=0)


def side_by_side(x, rows):
    return jnp.concatenate([x[rows * h : rows * (h + 1)] for h in range(x.shape[0] // rows)], axis=1)


def attend_kernel(q_ref, kv_ref, seg_ref, at_ref, all_ref, o_ref, p_ref):
    rows = q_ref.shape[0]
    kv = kv_ref[...].reshape(-1, 2 * HD)
    key, value = kv[:, :HD], kv[:, HD:]
    query = stacked(q_ref[...])
    heads = query.shape[0] // rows
    scores = lax.dot_general(query, key, (((1,), (1,)), ((), ())), preferred_element_type=F32)
    scores = (scores * (1.0 / math.sqrt(HD))).reshape(heads, rows, -1)
    key_at = lax.broadcasted_iota(jnp.int32, (rows, key.shape[0]), 1)
    allowed = jnp.logical_and(seg_ref[0] == all_ref[0], key_at <= at_ref[...])
    scores = jnp.where(allowed[None], scores, F32(-1e30))
    top = jnp.max(scores, axis=-1, keepdims=True)
    raised = jnp.exp(scores - top)
    weights = (raised * (1.0 / jnp.sum(raised, axis=-1, keepdims=True))).astype(BF16).reshape(heads * rows, -1)
    p_ref[0, 0] = weights
    mixed = jnp.dot(weights, value, preferred_element_type=F32)
    o_ref[...] = side_by_side(mixed, rows).astype(BF16)


def attend(q, kv, segments, own_seg, own_at, heads):
    batch, rows = own_seg.shape
    n_t, groups, span = kv.shape[0], kv.shape[2] // (2 * HD), segments.shape[1]
    q_spec = pl.BlockSpec((rows, heads * HD), lambda b, g: (b, g))
    return pl.pallas_call(
        attend_kernel,
        grid=(batch, groups),
        out_shape=[
            jax.ShapeDtypeStruct(q.shape, BF16),
            jax.ShapeDtypeStruct((batch, groups, heads * rows, span), BF16),
        ],
        in_specs=[
            q_spec,
            pl.BlockSpec((n_t, rows, 2 * HD), lambda b, g: (0, b, g)),
            pl.BlockSpec((1, rows, 1), lambda b, g: (b, 0, 0)),
            pl.BlockSpec((rows, 1), lambda b, g: (0, 0)),
            pl.BlockSpec((1, 1, span), lambda b, g: (b, 0, 0)),
        ],
        out_specs=[q_spec, pl.BlockSpec((1, 1, heads * rows, span), lambda b, g: (b, g, 0, 0))],
    )(q, kv, own_seg[:, :, None], own_at[:, None], segments[:, None, :])


def attend_back_kernel(do_ref, q_ref, kv_ref, p_ref, table_ref, dq_ref, dkv_ref):
    rows = q_ref.shape[0]
    kv = kv_ref[...].reshape(-1, 2 * HD)
    key, value = kv[:, :HD], kv[:, HD:]
    query, grad = stacked(q_ref[...]), stacked(do_ref[...])
    weights_b = p_ref[0, 0]
    weights = weights_b.astype(F32)
    product = weights * lax.dot_general(grad, value, (((1,), (1,)), ((), ())), preferred_element_type=F32)
    total = jnp.sum(product, axis=-1, keepdims=True)
    grad_scores = ((product - weights * total) * (1.0 / math.sqrt(HD))).astype(BF16)
    grad_query = side_by_side(jnp.dot(grad_scores, key, preferred_element_type=F32), rows)
    table = table_ref[:, :384]
    for j in range(q_ref.shape[1] // 128):
        at = slice(128 * j, 128 * j + 128)
        dq_ref[:, at] = turn(grad_query[:, at], table, -1.0).astype(BF16)
    over_rows = (((0,), (0,)), ((), ()))
    pair = jnp.concatenate(
        [
            lax.dot_general(query, grad_scores, over_rows, preferred_element_type=F32),
            lax.dot_general(grad, weights_b, over_rows, preferred_element_type=F32),
        ],
        axis=0,
    )
    dkv_ref[...] = pair.T.astype(BF16).reshape(dkv_ref.shape)


def attend_back(grad, q, kv, weights, table, heads):
    batch, groups, _, span = weights.shape
    rows = q.shape[0] // batch
    n_t = kv.shape[0]
    q_spec = pl.BlockSpec((rows, heads * HD), lambda b, g: (b, g))
    kv_spec = pl.BlockSpec((n_t, rows, 2 * HD), lambda b, g: (0, b, g))
    return pl.pallas_call(
        attend_back_kernel,
        grid=(batch, groups),
        out_shape=[jax.ShapeDtypeStruct(q.shape, BF16), jax.ShapeDtypeStruct(kv.shape, BF16)],
        in_specs=[
            q_spec,
            q_spec,
            kv_spec,
            pl.BlockSpec((1, 1, heads * rows, span), lambda b, g: (b, g, 0, 0)),
            pl.BlockSpec((rows, table.shape[1]), lambda b, g: (b, 0)),
        ],
        out_specs=[q_spec, kv_spec],
    )(grad, q, kv, weights, table)


def pair_sum_kernel(n_t, parts_ref, table_ref, out_ref, landed, send_sem, recv_sem):
    me = lax.axis_index("tensor")
    barrier = pltpu.get_barrier_semaphore()
    for r in range(1, n_t):
        pl.semaphore_signal(barrier, inc=1, device_id={"tensor": (me + r) % n_t}, device_id_type=MESH)
    pl.semaphore_wait(barrier, n_t - 1)

    def copy(r):
        other = (me + r) % n_t
        return pltpu.make_async_remote_copy(
            src_ref=parts_ref.at[other],
            dst_ref=landed.at[n_t - r],
            send_sem=send_sem.at[r],
            recv_sem=recv_sem.at[n_t - r],
            device_id={"tensor": other},
            device_id_type=MESH,
        )

    for r in range(1, n_t):
        copy(r).start()
    for r in range(1, n_t):
        other = (me + r) % n_t
        pltpu.make_async_remote_copy(
            src_ref=landed.at[r],
            dst_ref=landed.at[r],
            send_sem=send_sem.at[r],
            recv_sem=recv_sem.at[r],
            device_id={"tensor": other},
            device_id_type=MESH,
        ).wait_recv()
    table = table_ref[:, 384:]
    for j in range(out_ref.shape[1] // 128):
        at = slice(128 * j, 128 * j + 128)
        total = parts_ref[me, :, at].astype(F32)
        for r in range(1, n_t):
            total = total + landed[r, :, at].astype(F32)
        out_ref[:, at] = turn(total, table, -1.0).astype(BF16)
    for r in range(1, n_t):
        copy(r).wait_send()


def pair_sum(parts, table, n_t, ident):
    vmem = pl.BlockSpec(memory_space=pltpu.VMEM)
    return pl.pallas_call(
        functools.partial(pair_sum_kernel, n_t),
        out_shape=jax.ShapeDtypeStruct(parts.shape[1:], BF16),
        in_specs=[vmem, vmem],
        out_specs=vmem,
        scratch_shapes=[
            pltpu.VMEM(parts.shape, BF16),
            pltpu.SemaphoreType.DMA((n_t,)),
            pltpu.SemaphoreType.DMA((n_t,)),
        ],
        compiler_params=pltpu.CompilerParams(collective_id=ident, has_side_effects=True),
    )(parts, table)


def rope_tables(segments, start, rows):
    own = lax.dynamic_slice_in_dim(segments, start, rows, axis=1)
    earlier = jnp.sum((segments[:, None, :] < own[:, :, None]).astype(jnp.int32), axis=2)
    position = (start + jnp.arange(rows, dtype=jnp.int32)[None, :] - earlier).astype(F32)
    frequency = jnp.exp(jnp.arange(HD // 2, dtype=F32) * (-2.0 * math.log(10000.0) / HD))
    angles = (position[..., None] * frequency).reshape(-1, HD // 2)
    cosine, sine = jnp.cos(angles), jnp.sin(angles)
    zero, one = jnp.zeros_like(sine), jnp.ones_like(sine)
    columns = [cosine] * 4 + [-sine, zero] * 2 + [zero, sine] * 2
    columns += [cosine] * 2 + [one] * 2 + [-sine, zero, zero, zero] + [zero, sine, zero, zero]
    return own, jnp.concatenate(columns, axis=1)


def norm_forward(rows, gain):
    inv_rms = lax.rsqrt(jnp.mean(rows * rows, axis=-1, keepdims=True) + NORM_EPS)
    return (rows * inv_rms * gain).astype(BF16), inv_rms


def norm_backward(rows, inv_rms, gain, upstream):
    weighted = upstream * gain
    back = inv_rms * weighted - rows * (inv_rms * inv_rms * inv_rms) * jnp.mean(
        weighted * rows, axis=-1, keepdims=True
    )
    return back, jnp.sum(upstream * rows * inv_rms, axis=0)


def dot_nt(left, right):
    return lax.dot_general(left, right, (((1,), (1,)), ((), ())), preferred_element_type=F32)


def dot_tn(left, right):
    return lax.dot_general(left, right, (((0,), (0,)), ((), ())), preferred_element_type=F32)


def dot_nn(left, right):
    return jnp.dot(left, right, preferred_element_type=F32)


def dp_scatter(x):
    return lax.psum_scatter(x, "dp", scatter_dimension=0, tiled=True)


def body(
    heads, layer_input, segments, gain_attn, w_qkv, w_out_t, gain_mlp, w_gate_up, w_down_t, cotangent
):
    n_dp, n_t = lax.axis_size("dp"), lax.axis_size("tensor")
    me_t = lax.axis_index("tensor")
    batch, rows, width = layer_input.shape
    tokens = batch * rows
    shard_d = w_qkv.shape[0]
    q_cols = heads * HD
    parts = Cube(n_dp).parts

    x = layer_input.reshape(tokens, width)
    grad_in = cotangent.reshape(tokens, width)

    gu_w = w_gate_up.reshape(shard_d, 2, -1, 128).transpose(0, 2, 1, 3).reshape(shard_d, -1)
    grad_b = grad_in.astype(BF16)
    mlp_w = jnp.concatenate([gu_w, w_down_t], axis=1)
    mlp_w = lax.all_gather(mlp_w, "dp", axis=0, tiled=True)
    w_local = w_qkv.reshape(shard_d, -1)
    gains = jnp.concatenate([gain_attn, gain_mlp]).astype(F32)
    gains = jnp.pad(gains, (0, 8 * parts * 128 - gains.shape[0])).reshape(8 * parts, 128)
    sources = [w_local[:, :q_cols], w_local[:, q_cols:], w_out_t, gains, grad_b]
    first = Gather(
        ["zd", "zd", "zd", "d", "z"], [0, 0, 0, 0, 1], [s.shape for s in sources], n_t, n_dp, 1
    )
    wq, wkv, wo, gains, grad_rows = first(*sources)
    gains = gains.reshape(n_dp, -1)[:, : 2 * shard_d].reshape(n_dp, 2, shard_d)
    g_attn = gains[:, 0].reshape(1, width)
    g_mlp = gains[:, 1].reshape(1, width)

    own_seg, table = rope_tables(segments, me_t * rows, rows)
    own_at = me_t * rows + jnp.arange(rows, dtype=jnp.int32)
    normed_attn, scale_attn = norm_forward(x, g_attn)
    query, pairs = rope(dot_nn(normed_attn, wq), dot_nn(normed_attn, wkv), table)
    (pairs,) = Gather(["z"], [0], [pairs.shape], n_t, n_dp, 2)(pairs)
    mixed, weights = attend(query, pairs, segments, own_seg, own_at, heads)
    residual = x + dot_nt(mixed, wo)

    normed_mlp, scale_mlp = norm_forward(residual, g_mlp)
    mlp_rows, hidden, grad_gu, back_parts, *out_parts = Mlp(n_t, 3)(normed_mlp, grad_rows, mlp_w)
    flat = n_t * tokens
    down_part = dot_tn(grad_rows.reshape(flat, width), hidden.reshape(flat, -1)).astype(BF16)
    down_part, mlp_rows = lax.optimization_barrier((down_part, mlp_rows))
    down_grad = dp_scatter(down_part)
    gate_up_part = dot_tn(mlp_rows.reshape(flat, width), grad_gu.reshape(flat, -1)).astype(BF16)
    gate_up_part, back_parts = lax.optimization_barrier((gate_up_part, back_parts))
    gate_up_grad = dp_scatter(gate_up_part)

    grad_normed = jnp.sum(back_parts.astype(F32), axis=0)
    back_mlp, gain_mlp_part = norm_backward(residual, scale_mlp, g_mlp, grad_normed)
    grad_resid = grad_in + back_mlp
    resid_b = grad_resid.astype(BF16)

    out_grad = dot_tn(resid_b, mixed).astype(BF16)
    grad_mixed = dot_nn(resid_b, wo).astype(BF16)
    grad_query, grad_pairs = attend_back(grad_mixed, query, pairs, weights, table, heads)
    grad_pairs = pair_sum(grad_pairs, table, n_t, 5)
    grad_pairs, out_parts = lax.optimization_barrier((grad_pairs, out_parts))
    moved = [out_parts[0]] + [
        lax.ppermute(out_parts[r], "tensor", [(i, (i + r) % n_t) for i in range(n_t)]) for r in range(1, n_t)
    ]
    q_grad = dot_tn(normed_attn, grad_query).astype(BF16)
    kv_grad = dot_tn(normed_attn, grad_pairs).astype(BF16)
    grad_normed_attn = dot_nt(grad_query, wq) + dot_nt(grad_pairs, wkv)
    back_attn, gain_attn_part = norm_backward(x, scale_attn, g_attn, grad_normed_attn)
    input_grad = grad_resid + back_attn

    gain_parts = jnp.stack([gain_attn_part.reshape(n_dp, -1), gain_mlp_part.reshape(n_dp, -1)], axis=1)
    gain_parts = gain_parts.reshape(n_dp, -1)
    gain_parts = jnp.pad(gain_parts, ((0, 0), (0, 8 * parts * 128 - gain_parts.shape[1]))).reshape(-1, 128)
    q_grad, kv_grad, out_grad, gain_grads = Scatter(["dz", "dz", "dz", "da"], [1, 1, 1, 1], n_t, n_dp, 4)(
        q_grad, kv_grad, out_grad, gain_parts
    )
    gain_grads = gain_grads.reshape(-1)[: 2 * shard_d]
    gain_first, gain_second = gain_grads[:shard_d], gain_grads[shard_d:]
    down_grad, gate_up_grad, q_grad, moved = lax.optimization_barrier((down_grad, gate_up_grad, q_grad, moved))
    output = residual
    for part in moved:
        output = output + part.astype(F32)
    gate_up_grad = gate_up_grad.astype(F32)
    qkv_grad = jnp.concatenate([q_grad, kv_grad], axis=1)
    return (
        output.reshape(layer_input.shape),
        input_grad.reshape(layer_input.shape),
        gain_first,
        qkv_grad.reshape(w_qkv.shape),
        out_grad,
        gain_second,
        gate_up_grad.reshape(w_gate_up.shape),
        down_grad.astype(F32),
    )


def solution(mesh):
    placed = (
        P("dp", "tensor", None),
        P("dp", None),
        P("dp"),
        P("dp", "tensor", None),
        P("dp", "tensor"),
        P("dp"),
        P("dp", None, "tensor"),
        P("dp", "tensor"),
        P("dp", "tensor", None),
    )

    def whole(*args):
        heads = args[3].shape[2] // HD - 2
        return jax.shard_map(
            functools.partial(body, heads),
            mesh=mesh,
            in_specs=placed,
            out_specs=(placed[0], placed[0], P("dp"), placed[3], placed[4], P("dp"), placed[6], placed[7]),
            check_vma=False,
        )(*args)

    return whole
```

```python
import functools
import math

import jax
import jax.numpy as jnp
from jax import lax
from jax.experimental import pallas as pl
from jax.experimental.pallas import tpu as pltpu
from jax.sharding import PartitionSpec as P

HD = 64
NORM_EPS = 1e-05
F32 = jnp.float32
BF16 = jnp.bfloat16
MESH = pl.DeviceIdType.MESH
LATE = 2


class Cube:
    def __init__(self, size):
        self.size = size
        self.bits = size.bit_length() - 1
        assert 1 << self.bits == size and self.bits >= 1
        self.shape = (2,) * self.bits
        outer = list(range(1, self.bits))
        self.steps = len(outer)
        self.parts = max(1, self.steps)
        self.orders = [outer[p:] + outer[:p] for p in range(self.parts)]

    def own(self, bit):
        return lax.axis_index("dp") // (1 << bit) % 2

    def partner(self, bit):
        return lax.axis_index("dp") + (1 << bit) * (1 - 2 * self.own(bit))

    def index(self, free, flipped=()):
        spots = []
        for bit in reversed(range(self.bits)):
            if bit in free:
                spots.append(slice(None))
            else:
                spots.append(1 - self.own(bit) if bit in flipped else self.own(bit))
        return tuple(spots)

    def cuts(self, rows):
        count = rows // self.parts
        return [pl.ds(part * count, count) for part in range(self.parts)]

    def move(self, step, part):
        if step == self.steps:
            return tuple(range(1, self.bits)), 0
        return tuple(self.orders[part][:step]), self.orders[part][step]

    def keys(self, step):
        return [(step, part) for part in range(self.parts if step < self.steps else 1)]

    def row(self, key):
        return key[0] * self.parts + key[1]


class Gather:
    def __init__(self, kinds, late, shapes, n_t, n_dp, ident, work=None):
        self.work = work
        self.more_in, self.more_out = (work.more_in, work.more_out) if work else (0, 0)
        self.kinds, self.late, self.shapes = kinds, late, shapes
        self.n_t, self.cube, self.ident = n_t, Cube(n_dp), ident
        self.ticks = [[("own", 0)]] + [[("up", k), ("down", k)] for k in range(1, n_t)]
        self.insts = [inst for tick in self.ticks for inst in tick]
        self.uses_dp = any("d" in kind for kind in kinds)
        self.uses_z = any("z" in kind for kind in kinds)
    def out_shape(self, a):
        rows, cols = self.shapes[a]
        kind = self.kinds[a]
        if kind == "z":
            return (self.n_t, rows, cols)
        return self.cube.shape + (rows, cols * (self.n_t if "z" in kind else 1))

    def place(self, ref, a, z, free=(), flipped=(), part=None):
        rows, cols = self.shapes[a]
        kind = self.kinds[a]
        if kind == "z":
            return ref.at[z]
        span = pl.ds(0, rows) if part is None else self.cube.cuts(rows)[part]
        width = pl.ds(pl.multiple_of(z * cols, cols), cols) if "z" in kind else pl.ds(0, cols)
        return ref.at[self.cube.index(free, flipped) + (span, width)]

    def kernel(self, *refs):
        count = len(self.kinds)
        more_in, more_out = self.more_in, self.more_out
        srcs, given = refs[:count], refs[count : count + more_in]
        refs = refs[count + more_in :]
        dests, wanted, scratch = refs[:count], refs[count : count + more_out], refs[count + more_out + 5 :]
        own_sem, z_send, z_recv, d_send, d_recv = refs[count + more_out : count + more_out + 5]
        n_t, cube = self.n_t, self.cube
        me_t = lax.axis_index("tensor")
        main = [a for a in range(count) if not self.late[a]]
        tail = [a for a in range(count) if self.late[a]]

        barrier = pltpu.get_barrier_semaphore()
        if self.uses_dp:
            for bit in range(cube.bits):
                pl.semaphore_signal(barrier, inc=1, device_id={"dp": cube.partner(bit)}, device_id_type=MESH)
        peers = self.n_t - 1 if self.uses_z else 0
        for r in range(peers):
            pl.semaphore_signal(barrier, inc=1, device_id={"tensor": (me_t + 1 + r) % n_t}, device_id_type=MESH)
        pl.semaphore_wait(barrier, peers + (cube.bits if self.uses_dp else 0))

        def own_copy(a):
            return pltpu.make_async_copy(srcs[a], self.place(dests[a], a, me_t), own_sem.at[a])

        for a in range(count):
            own_copy(a).start()

        def piece_of(inst):
            way, k = inst
            return me_t if way == "own" else me_t - k if way == "up" else me_t + k

        def exists(inst, fn):
            way, k = inst
            if way == "own":
                fn()
            elif way == "up":
                pl.when(me_t >= k)(fn)
            else:
                pl.when(me_t + k < n_t)(fn)

        def z_copy(a, way, k, src):
            piece = me_t - (k - 1) if way == "up" else me_t + (k - 1)
            index = 2 * (k - 1) + (way == "down")
            dest = self.place(dests[a], a, piece)
            return pltpu.make_async_remote_copy(
                src_ref=dest if src is None else src,
                dst_ref=dest,
                send_sem=z_send.at[a, index],
                recv_sem=z_recv.at[a, index],
                device_id={"tensor": me_t + 1 if way == "up" else me_t - 1},
                device_id_type=MESH,
            )

        def z_cond(way, k):
            return (
                jnp.logical_and(me_t >= k - 1, me_t < n_t - 1)
                if way == "up"
                else jnp.logical_and(me_t + (k - 1) < n_t, me_t > 0)
            )

        def z_start(a, inst):
            way, k = inst
            for out_way in ("up", "down") if way == "own" else (way,):
                if k + 1 < n_t:

                    @pl.when(z_cond(out_way, k + 1))
                    def _():
                        z_copy(a, out_way, k + 1, srcs[a] if way == "own" else None).start()

        def z_arrive(a, inst):
            way, k = inst
            if way != "own":
                index = 2 * (k - 1) + (way == "down")
                dest = self.place(dests[a], a, piece_of(inst))
                pltpu.make_async_remote_copy(
                    src_ref=dest,
                    dst_ref=dest,
                    send_sem=z_send.at[a, index],
                    recv_sem=z_recv.at[a, index],
                    device_id={"tensor": me_t},
                    device_id_type=MESH,
                ).wait_recv()

        def d_copy(a, inst, key, incoming=False):
            free, bit = cube.move(*key)
            part = key[1] if key[0] < cube.steps else None
            spot = self.place(dests[a], a, piece_of(inst), free, (bit,) if incoming else (), part)
            sem = (a, self.insts.index(inst), cube.row(key))
            return pltpu.make_async_remote_copy(
                src_ref=spot,
                dst_ref=spot,
                send_sem=d_send.at[sem],
                recv_sem=d_recv.at[sem],
                device_id={"dp": cube.partner(bit)},
                device_id_type=MESH,
            )

        def d_advance(a, inst, stage):
            if stage == 0 and inst[0] == "own":
                own_copy(a).wait()
            if stage > 0:
                for key in cube.keys(stage - 1):
                    d_copy(a, inst, key, True).wait_recv()
            if stage <= cube.steps:
                for key in cube.keys(stage):
                    d_copy(a, inst, key).start()

        def in_dp(a, inst):
            return "d" in self.kinds[a] and (inst[0] == "own" or "z" in self.kinds[a])

        def stage(a, now):
            for inst in self.ticks[now]:

                def move(inst=inst):
                    z_arrive(a, inst)
                    z_start(a, inst)

                exists(inst, move)

        def plan():
            z_main = [a for a in main if "z" in self.kinds[a]]
            z_tail = [a for a in tail if "z" in self.kinds[a]]
            length = n_t if self.uses_z else 1
            total = max(length + cube.steps + 2, 2 * length + 1)
            for now in range(total):
                for inst in self.ticks[now] if now < length else ():
                    def arrive(inst=inst):
                        for a in z_main:
                            z_arrive(a, inst)
                            z_start(a, inst)
                        for a in main:
                            if in_dp(a, inst):
                                d_advance(a, inst, 0)

                    exists(inst, arrive)
                late_now = now - length + LATE
                if 0 <= late_now < length and z_tail:
                    for inst in self.ticks[late_now]:
                        def arrive_late(inst=inst):
                            for a in z_tail:
                                z_arrive(a, inst)
                                z_start(a, inst)

                        exists(inst, arrive_late)
                for age in range(1, cube.steps + 2):
                    tick = now - age
                    for inst in self.ticks[tick] if 0 <= tick < length else ():
                        def advance(inst=inst, age=age):
                            for a in main:
                                if in_dp(a, inst):
                                    d_advance(a, inst, age)

                        exists(inst, advance)

        if self.work is not None:
            self.work(
                stage, lambda a, age: d_advance(a, ("own", 0), age), own_copy, given, dests, wanted, scratch
            )
        else:
            plan()

        for inst in self.insts:
            def drain(inst=inst):
                for a in main:
                    if in_dp(a, inst):
                        for stage in range(cube.steps + 1):
                            for key in cube.keys(stage):
                                d_copy(a, inst, key).wait_send()

            exists(inst, drain)
        for a in range(count):
            if "z" in self.kinds[a]:
                for k in range(1, n_t):
                    for way in ("up", "down"):

                        @pl.when(z_cond(way, k))
                        def _():
                            z_copy(a, way, k, srcs[a] if k == 1 else None).wait_send()

            if not in_dp(a, ("own", 0)) and not (self.work and a == 0):
                own_copy(a).wait()

    def __call__(self, *arrays, given=()):
        count, work = len(arrays), self.work
        vmem, anywhere = pl.BlockSpec(memory_space=pltpu.VMEM), pl.BlockSpec(memory_space=pl.ANY)
        n_z = max(1, 2 * (self.n_t - 1))
        rows = (self.cube.steps + 1) * self.cube.parts
        insts = len(self.insts) if self.uses_dp else 1
        outs = pl.pallas_call(
            self.kernel,
            out_shape=[jax.ShapeDtypeStruct(self.out_shape(a), arrays[a].dtype) for a in range(count)]
            + (work.out_shape if work else []),
            in_specs=[vmem] * count + (work.in_specs if work else []),
            out_specs=[vmem if work and a == 0 else anywhere for a in range(count)] + (work.out_specs if work else []),
            scratch_shapes=[
                pltpu.SemaphoreType.DMA((count,)),
                pltpu.SemaphoreType.DMA((count, n_z)),
                pltpu.SemaphoreType.DMA((count, n_z)),
                pltpu.SemaphoreType.DMA((count, insts, rows)),
                pltpu.SemaphoreType.DMA((count, insts, rows)),
            ]
            + (work.scratch if work else []),
            compiler_params=pltpu.CompilerParams(
                collective_id=self.ident, has_side_effects=True, vmem_limit_bytes=60 << 20
            ),
        )(*arrays, *given)
        return [
            out.reshape(-1, out.shape[-1]) if "d" in kind else out for out, kind in zip(outs, self.kinds)
        ] + list(outs[count:])


class Scatter:
    def __init__(self, kinds, pieces, n_t, n_dp, ident):
        self.kinds = kinds
        self.pieces = [n_t if kind == "dz" else count for kind, count in zip(kinds, pieces)]
        self.n_t, self.cube, self.ident = n_t, Cube(n_dp), ident

    def kernel(self, *refs):
        count = len(self.kinds)
        n_t, cube = self.n_t, self.cube
        grads, outs = refs[:count], refs[count : 2 * count]
        core_in, z_in = refs[2 * count : 3 * count], refs[3 * count : 4 * count]
        step_in = [refs[4 * count + a * cube.steps :][: cube.steps] for a in range(count)]
        d_send, d_recv, z_send, z_recv = refs[-4:]
        me_t = lax.axis_index("tensor")
        to_z = any(kind != "d" for kind in self.kinds)

        barrier = pltpu.get_barrier_semaphore()
        for bit in range(cube.bits):
            pl.semaphore_signal(barrier, inc=1, device_id={"dp": cube.partner(bit)}, device_id_type=MESH)
        if to_z:
            for r in range(1, n_t):
                pl.semaphore_signal(barrier, inc=1, device_id={"tensor": (me_t + r) % n_t}, device_id_type=MESH)
        pl.semaphore_wait(barrier, cube.bits + (n_t - 1 if to_z else 0))

        def columns(a, i):
            width = grads[a].shape[-1] // self.pieces[a]
            if self.kinds[a] == "dz":
                return pl.ds(pl.multiple_of((me_t + n_t - 1 - i) % n_t * width, width), width)
            return pl.ds(i * width, width)

        def blocks(a, i, key, flipped=()):
            free, bit = cube.move(*key)
            rows = grads[a].shape[-2]
            span = cube.cuts(rows)[key[1]] if key[0] < cube.steps else pl.ds(0, rows)
            return grads[a].at[cube.index(free, flipped) + (span, columns(a, i))]

        def mine(a, i):
            return grads[a].at[cube.index(()) + (pl.ds(0, grads[a].shape[-2]), columns(a, i))]

        def landing(a, i, key):
            step, part = key
            if step == cube.steps:
                return core_in[a].at[i]
            return step_in[a][step].at[i, part]

        def d_copy(a, i, key):
            free, bit = cube.move(*key)
            return pltpu.make_async_remote_copy(
                src_ref=blocks(a, i, key, (bit,)),
                dst_ref=landing(a, i, key),
                send_sem=d_send.at[a, i, cube.row(key)],
                recv_sem=d_recv.at[a, i, cube.row(key)],
                device_id={"dp": cube.partner(bit)},
                device_id_type=MESH,
            )

        def add(a, i, key):
            free, bit = cube.move(*key)
            source = landing(a, i, key)
            rows = source.shape[-2]
            block = 16 if rows % 16 == 0 else 8
            first = cube.cuts(grads[a].shape[-2])[key[1]].start if key[0] < cube.steps else 0
            for number in range(1 << len(free)):
                held = sorted(free, reverse=True)
                bits = {b: number >> (len(held) - 1 - j) & 1 for j, b in enumerate(held)}
                target = grads[a].at[tuple(bits.get(b, cube.own(b)) for b in reversed(range(cube.bits)))]
                given = source.at[tuple(bits[b] for b in held)]

                def one(j, carry):
                    at = pl.ds(pl.multiple_of(j * block, block), block)
                    spot = (pl.ds(pl.multiple_of(first + j * block, block), block), columns(a, i))
                    target[spot] = (target[spot].astype(F32) + given[at, :].astype(F32)).astype(target.dtype)
                    return carry

                lax.fori_loop(0, rows // block, one, 0)

        def z_copy(a, i):
            other = (me_t + n_t - 1 - i) % n_t
            return pltpu.make_async_remote_copy(
                src_ref=mine(a, i if self.kinds[a] == "dz" else 0),
                dst_ref=z_in[a].at[me_t],
                send_sem=z_send.at[a, i],
                recv_sem=z_recv.at[a, me_t],
                device_id={"tensor": other},
                device_id_type=MESH,
            )

        def z_wait(a, r):
            other = (me_t + r) % n_t
            pltpu.make_async_remote_copy(
                src_ref=z_in[a].at[other],
                dst_ref=z_in[a].at[other],
                send_sem=z_send.at[a, 0],
                recv_sem=z_recv.at[a, other],
                device_id={"tensor": other},
                device_id_type=MESH,
            ).wait_recv()

        def advance(a, i, age):
            if age > 0:
                for key in cube.keys(cube.steps + 1 - age):
                    d_copy(a, i, key).wait_recv()
                    add(a, i, key)
            if age <= cube.steps:
                for key in cube.keys(cube.steps - age):
                    d_copy(a, i, key).start()
                return
            kind = self.kinds[a]
            if kind == "d":
                outs[a][:, columns(a, i)] = mine(a, i)[...].astype(F32)
            elif kind == "dz":
                if i < n_t - 1:
                    z_copy(a, i).start()
            else:
                for r in range(n_t - 1):
                    z_copy(a, r).start()

        most = max(self.pieces)
        order = range(count)
        for a in order:
            advance(a, 0, 0)
        for now in range(most + cube.steps + 1):
            for a in order:
                if now + 1 < self.pieces[a]:
                    advance(a, now + 1, 0)
            for age in range(cube.steps + 1, 0, -1):
                i = now + 1 - age
                for a in order:
                    if 0 <= i < self.pieces[a]:
                        advance(a, i, age)
        for a in order:
            if self.kinds[a] == "dz":
                for r in range(1, n_t):
                    z_wait(a, r)
                own = mine(a, n_t - 1)
                block = 16

                def total(j, carry, a=a, own=own):
                    at = pl.ds(pl.multiple_of(j * block, block), block)
                    value = own[at, :].astype(F32)
                    for r in range(1, n_t):
                        value = value + z_in[a][(me_t + r) % n_t, at, :].astype(F32)
                    outs[a][at, :] = value
                    return carry

                lax.fori_loop(0, own.shape[0] // block, total, 0)
            elif self.kinds[a] == "da":
                z_in[a][me_t] = mine(a, 0)[...]
                for r in range(1, n_t):
                    z_wait(a, r)
                value = z_in[a][0]
                for z in range(1, n_t):
                    value = value + z_in[a][z]
                outs[a][...] = value
        for a in order:
            for i in range(self.pieces[a]):
                for step in range(cube.steps + 1):
                    for key in cube.keys(step):
                        d_copy(a, i, key).wait_send()
            if self.kinds[a] != "d":
                for i in range(n_t - 1):
                    z_copy(a, i).wait_send()

    def __call__(self, *grads):
        count = len(grads)
        cube, n_t = self.cube, self.n_t
        outs, core, step, z = [], [], [], []
        for grad, kind, pieces in zip(grads, self.kinds, self.pieces):
            rows, cols = grad.shape[0] // cube.size, grad.shape[1] // pieces
            outs.append(jax.ShapeDtypeStruct((rows, cols if kind == "dz" else grad.shape[1]), F32))
            core.append(pltpu.VMEM((pieces,) + (2,) * cube.steps + (rows, cols), grad.dtype))
            for k in range(cube.steps):
                step.append(pltpu.VMEM((pieces, cube.parts) + (2,) * k + (rows // cube.parts, cols), grad.dtype))
            slots = (1, 8, 128) if kind == "d" else (n_t, rows, cols)
            z.append(pltpu.VMEM(slots, grad.dtype))
        most = max(self.pieces)
        keys = (cube.steps + 1) * cube.parts
        grads = [grad.reshape(cube.shape + (-1, grad.shape[1])) for grad in grads]
        return pl.pallas_call(
            self.kernel,
            out_shape=outs,
            in_specs=[pl.BlockSpec(memory_space=pltpu.VMEM)] * count,
            out_specs=[pl.BlockSpec(memory_space=pltpu.VMEM)] * count,
            scratch_shapes=core
            + z
            + step
            + [
                pltpu.SemaphoreType.DMA((count, most, keys)),
                pltpu.SemaphoreType.DMA((count, most, keys)),
                pltpu.SemaphoreType.DMA((count, n_t)),
                pltpu.SemaphoreType.DMA((count, n_t)),
            ],
            compiler_params=pltpu.CompilerParams(
                collective_id=self.ident, has_side_effects=True, vmem_limit_bytes=60 << 20
            ),
        )(*grads)


class Mlp:
    def __init__(self, n_t, ident):
        self.n_t, self.ident = n_t, ident

    def kernel(
        self, rows_ref, low_ref, high_ref, gu_hbm, down_hbm, all_ref, grads_ref, hid_ref, dgu_ref, back_ref, *refs
    ):
        out_refs = refs[: self.n_t]
        (gu, down, held, dy, dh, hid, dgu, flat, back, out, own_sem, w_sem, dy_sem, put_sem, z_send, z_recv, b_send, b_recv) = refs[self.n_t :]
        n_t = self.n_t
        me = lax.axis_index("tensor")
        units = down.shape[1]
        width = rows_ref.shape[1]
        interior = jnp.logical_and(me > 0, me < n_t - 1)

        barrier = pltpu.get_barrier_semaphore()
        for r in range(1, n_t):
            pl.semaphore_signal(barrier, inc=1, device_id={"tensor": (me + r) % n_t}, device_id_type=MESH)
        down_copy = pltpu.make_async_copy(down_hbm, down, w_sem.at[0])
        down_copy.start()

        gu_copies = [
            pltpu.make_async_copy(
                gu_hbm.at[:, pl.ds(half * units + 128 * t, 128)],
                gu.at[:, pl.ds(256 * t + 128 * half, 128)],
                w_sem.at[1 + 2 * t + half],
            )
            for t in range(units // 128)
            for half in (0, 1)
        ]
        for copy in gu_copies:
            copy.start()
        own_copy = pltpu.make_async_copy(rows_ref, held.at[me], own_sem)
        own_copy.start()

        def order(i):
            low, high = me, n_t - 1 - me
            both = 2 * jnp.minimum(low, high)
            near = i <= both
            distance = jnp.where(near, (i + 1) // 2, i - both // 2)
            way = jnp.where(near, (i + 1) % 2, jnp.where(low > high, 0, 1))
            return distance, way, jnp.where(way == 0, me - distance, me + distance)

        def piece_of(i):
            return order(i)[2]

        def hop(distance, way, piece, src=None):
            index = 2 * (distance - 1) + way
            return pltpu.make_async_remote_copy(
                src_ref=held.at[piece] if src is None else src,
                dst_ref=held.at[piece],
                send_sem=z_send.at[index],
                recv_sem=z_recv.at[index],
                device_id={"tensor": me + 1 - 2 * way},
                device_id_type=MESH,
            )

        def may_send(distance, way):
            room = jnp.where(way == 0, n_t - 1 - me, me)
            behind = jnp.where(way == 0, me, n_t - 1 - me)
            return jnp.logical_and(room > 0, behind >= distance - 1)

        def arrive(i):
            distance, way, piece = order(i)
            hop(distance, way, piece).wait_recv()

            @pl.when(may_send(distance + 1, way))
            def _():
                hop(distance + 1, way, piece).start()

        def dy_copies(i):
            part = low_ref.shape[1]
            return [
                pltpu.make_async_copy(ref.at[piece_of(i)], dy.at[i % 2, pl.ds(k * part, part), :], dy_sem.at[i % 2, k])
                for k, ref in enumerate((low_ref, high_ref))
            ]

        def dy_keep(i):
            return pltpu.make_async_copy(dy.at[i % 2], grads_ref.at[piece_of(i)], dy_sem.at[2, 0])

        def puts(i):
            piece, slot = piece_of(i), i % 2
            return [
                pltpu.make_async_copy(hid.at[slot], hid_ref.at[piece], put_sem.at[slot, 0]),
                pltpu.make_async_copy(flat.at[slot], dgu_ref.at[piece], put_sem.at[slot, 1]),
            ]

        def out_put(i, r=0):
            return pltpu.make_async_copy(out.at[i % 2], out_refs[r], put_sem.at[i % 2, 2])

        def put_start(i):
            for put in puts(i):
                put.start()
            for r in range(n_t):

                @pl.when((piece_of(i) - me + n_t) % n_t == r)
                def _():
                    out_put(i, r).start()

        def put_wait(i):
            for put in puts(i):
                put.wait()
            out_put(i).wait()

        def keep(i):
            return pltpu.make_async_copy(held.at[piece_of(i)], all_ref.at[piece_of(i)], own_sem)

        def back_copy(i):
            piece = piece_of(i)
            return pltpu.make_async_remote_copy(
                src_ref=back.at[i],
                dst_ref=back_ref.at[me],
                send_sem=b_send.at[i],
                recv_sem=b_recv.at[me],
                device_id={"tensor": piece},
                device_id_type=MESH,
            )

        for copy in dy_copies(0):
            copy.start()
        pl.semaphore_wait(barrier, n_t - 1)
        for way in (0, 1):

            @pl.when(may_send(1, way))
            def _():
                hop(1, way, me, rows_ref).start()

        own_copy.wait()
        down_copy.wait()
        wide = units // 256

        def chunk(i, carry):
            slot = i % 2
            piece = piece_of(i)

            @pl.when(jnp.logical_and(i > 0, jnp.logical_not(interior)))
            def _():
                arrive(i)

            @pl.when(jnp.logical_and(i == 1, interior))
            def _():
                arrive(i)

            @pl.when(jnp.logical_and(jnp.logical_and(i > 0, i + 1 < n_t), interior))
            def _():
                arrive(i + 1)

            @pl.when(i + 1 < n_t)
            def _():
                for copy in dy_copies(i + 1):
                    copy.start()

            @pl.when(i >= 2)
            def _():
                put_wait(i - 2)

            for copy in dy_copies(i):
                copy.wait()
            keep(i).start()
            dy_keep(i).start()

            def grad_tile(t, c):
                at = pl.ds(pl.multiple_of(t * 256, 256), 256)
                dh[:, at] = jnp.dot(dy[slot], down[:, at], preferred_element_type=F32)
                return c

            lax.fori_loop(0, wide, grad_tile, 0)
            if units % 256:
                dh[:, wide * 256 :] = jnp.dot(dy[slot], down[:, wide * 256 :], preferred_element_type=F32)

            @pl.when(i == 0)
            def _():
                for copy in gu_copies:
                    copy.wait()

            def unit_tile(t, c):
                at = pl.ds(pl.multiple_of(t * 128, 128), 128)
                pair = jnp.dot(held[piece], gu[:, pl.ds(pl.multiple_of(t * 256, 256), 256)], preferred_element_type=F32)
                gate, up = pair[:, :128], pair[:, 128:]
                sigmoid = jax.nn.sigmoid(gate)
                active = gate * sigmoid
                grad = dh[:, at]
                hid[slot, :, at] = (active * up).astype(BF16)
                first = (grad * up * sigmoid * (1.0 + gate * (1.0 - sigmoid))).astype(BF16)
                second = (grad * active).astype(BF16)
                dgu[slot, :, pl.ds(pl.multiple_of(t * 256, 128), 128)] = first
                dgu[slot, :, pl.ds(pl.multiple_of(t * 256 + 128, 128), 128)] = second
                flat[slot, :, at] = first
                flat[slot, :, pl.ds(pl.multiple_of(units + t * 128, 128), 128)] = second
                return c

            lax.fori_loop(0, units // 128, unit_tile, 0)

            def back_tile(j, c):
                at = pl.ds(pl.multiple_of(j * 256, 256), 256)
                value = lax.dot_general(dgu[slot], gu[at, :], (((1,), (1,)), ((), ())), preferred_element_type=F32)
                back[i, :, at] = value.astype(BF16)
                return c

            lax.fori_loop(0, width // 256, back_tile, 0)

            @pl.when(i > 0)
            def _():
                back_copy(i).start()

            def out_tile(j, c):
                at = pl.ds(pl.multiple_of(j * 256, 256), 256)
                value = lax.dot_general(hid[slot], down[at, :], (((1,), (1,)), ((), ())), preferred_element_type=F32)
                out[slot, :, at] = value.astype(BF16)
                return c

            lax.fori_loop(0, width // 256, out_tile, 0)
            put_start(i)
            keep(i).wait()
            dy_keep(i).wait()
            return carry

        lax.fori_loop(0, n_t, chunk, 0)
        mine = pltpu.make_async_copy(back.at[0], back_ref.at[me], own_sem)
        mine.start()
        for i in range(max(0, n_t - 2), n_t):
            put_wait(i)
        for r in range(1, n_t):
            other = (me + r) % n_t
            pltpu.make_async_remote_copy(
                src_ref=back_ref.at[other],
                dst_ref=back_ref.at[other],
                send_sem=b_send.at[0],
                recv_sem=b_recv.at[other],
                device_id={"tensor": other},
                device_id_type=MESH,
            ).wait_recv()
        mine.wait()
        for i in range(1, n_t):
            back_copy(i).wait_send()
        for k in range(1, n_t):
            for way in (0, 1):

                @pl.when(may_send(k, way))
                def _():
                    hop(k, way, me, rows_ref).wait_send()

    def __call__(self, rows, low, high, w_gu, w_down):
        n_t = self.n_t
        tokens, width = rows.shape
        units = w_down.shape[1]
        hops = max(1, 2 * (n_t - 1))
        any_spec = pl.BlockSpec(memory_space=pl.ANY)

        def held(*shape):
            return pltpu.VMEM(shape, BF16)

        def put(cols, *lead):
            return jax.ShapeDtypeStruct(lead + (tokens, cols), BF16)

        return pl.pallas_call(
            self.kernel,
            out_shape=[put(width, n_t), put(width, n_t), put(units, n_t), put(2 * units, n_t), put(width, n_t)] + [put(width)] * n_t,
            in_specs=[pl.BlockSpec(memory_space=pltpu.VMEM)] + [any_spec] * 4,
            out_specs=[any_spec] * (5 + n_t),
            scratch_shapes=[
                held(width, 2 * units),
                held(width, units),
                held(n_t, tokens, width),
                held(2, tokens, width),
                pltpu.VMEM((tokens, units), F32),
                held(2, tokens, units),
                held(2, tokens, 2 * units),
                held(2, tokens, 2 * units),
                held(n_t, tokens, width),
                held(2, tokens, width),
                pltpu.SemaphoreType.DMA,
                pltpu.SemaphoreType.DMA((1 + units // 64,)),
                pltpu.SemaphoreType.DMA((3, 2)),
                pltpu.SemaphoreType.DMA((2, 3)),
                pltpu.SemaphoreType.DMA((hops,)),
                pltpu.SemaphoreType.DMA((hops,)),
                pltpu.SemaphoreType.DMA((n_t,)),
                pltpu.SemaphoreType.DMA((n_t,)),
            ],
            compiler_params=pltpu.CompilerParams(
                collective_id=self.ident, has_side_effects=True, vmem_limit_bytes=60 << 20
            ),
        )(rows, low, high, w_gu, w_down)


def turn(x, table, sign):
    cosine, low, high = table[:, :128], table[:, 128:256], table[:, 256:]
    return x * cosine + sign * (pltpu.roll(x, 96, 1) * low + pltpu.roll(x, 32, 1) * high)


def rope_kernel(kv_ref, table_ref, kvo_ref):
    for j in range(kv_ref.shape[1] // 128):
        at = slice(128 * j, 128 * j + 128)
        kvo_ref[:, at] = turn(kv_ref[:, at], table_ref[:, 384:], 1.0).astype(BF16)


def rope(kv, table):
    vmem = pl.BlockSpec(memory_space=pltpu.VMEM)
    return pl.pallas_call(
        rope_kernel, out_shape=jax.ShapeDtypeStruct(kv.shape, BF16), in_specs=[vmem, vmem], out_specs=vmem
    )(kv, table)


def stacked(x):
    return jnp.concatenate([x[:, HD * h : HD * (h + 1)] for h in range(x.shape[1] // HD)], axis=0)


def side_by_side(x, rows):
    return jnp.concatenate([x[rows * h : rows * (h + 1)] for h in range(x.shape[0] // rows)], axis=1)


class Attend:
    more_in, more_out = 9, 5

    def __init__(self, cube, n_t, batch, rows, heads, groups, span, width):
        self.cube, self.n_t, self.batch, self.rows, self.heads, self.groups = cube, n_t, batch, rows, heads, groups
        steps, tokens, inner = batch * groups, batch * rows, groups * heads * HD
        self.out_shape = [
            jax.ShapeDtypeStruct((tokens, inner), BF16),
            jax.ShapeDtypeStruct((tokens, inner), BF16),
            jax.ShapeDtypeStruct((tokens, width), F32),
            jax.ShapeDtypeStruct((tokens, width), BF16),
            jax.ShapeDtypeStruct((steps, heads * rows, span), BF16),
        ]
        self.out_specs = [pl.BlockSpec(memory_space=pltpu.VMEM)] * 4 + [pl.BlockSpec(memory_space=pl.ANY)]
        self.scratch = [
            pltpu.VMEM((steps, heads * rows, span), BF16),
            pltpu.SemaphoreType.DMA((steps,)),
            pltpu.VMEM((width, inner), BF16),
            pltpu.VMEM((width, inner), BF16),
            pltpu.SemaphoreType.DMA((2,)),
        ]
        vmem = pl.BlockSpec(memory_space=pltpu.VMEM)
        self.in_specs = [vmem] * 7 + [pl.BlockSpec(memory_space=pl.ANY)] * 2

    def __call__(self, stage, advance, own_copy, given, dests, wanted, scratch):
        n_ref, table_ref, x_ref, gain_ref, seg_ref, at_ref, all_ref, wq_hbm, wo_hbm = given
        q_ref, o_ref, h_ref, next_ref, p_ref = wanted
        held, sem, wq, wo, w_sem = scratch
        kv_ref = dests[0]
        rows, heads, groups = self.rows, self.heads, self.groups
        last = self.cube.steps + 1
        wq_copy = pltpu.make_async_copy(wq_hbm, wq, w_sem.at[0])
        wo_copy = pltpu.make_async_copy(wo_hbm, wo, w_sem.at[1])
        stage(0, 0)
        wq_copy.start()
        advance(1, 0)
        advance(2, 0)
        wo_copy.start()

        def query_tile(t, carry):
            at = pl.ds(pl.multiple_of(t * 256, 256), 256)
            value = jnp.dot(n_ref[...], wq[:, at], preferred_element_type=F32)
            for half in (0, 1):
                place = pl.ds(pl.multiple_of(t * 256 + half * 128, 128), 128)
                q_ref[:, place] = turn(value[:, 128 * half : 128 * half + 128], table_ref[:, :384], 1.0).astype(BF16)
            return carry

        half = wq.shape[1] // 512
        if self.n_t > 1:
            stage(0, 1)
        stage(3, 0)
        wq_copy.wait()
        lax.fori_loop(0, half, query_tile, 0)
        if self.n_t > 2:
            stage(0, 2)
        advance(1, 1)
        lax.fori_loop(half, 2 * half, query_tile, 0)
        for tick in range(3, self.n_t):
            stage(0, tick)
        own_copy(0).wait()
        advance(2, 1)
        if self.n_t > 1:
            stage(3, 1)

        def put(j):
            return pltpu.make_async_copy(held.at[j], p_ref.at[j], sem.at[j])

        def step(j, carry):
            b, g = j // groups, j % groups
            own = pl.ds(pl.multiple_of(b * rows, rows), rows)
            columns = pl.ds(pl.multiple_of(g * heads * HD, 128), heads * HD)
            kv = kv_ref[:, own, pl.ds(pl.multiple_of(g * 2 * HD, 2 * HD), 2 * HD)].reshape(-1, 2 * HD)
            key, value = kv[:, :HD], kv[:, HD:]
            scores = lax.dot_general(
                stacked(q_ref[own, columns]), key, (((1,), (1,)), ((), ())), preferred_element_type=F32
            )
            scores = (scores * (1.0 / math.sqrt(HD))).reshape(heads, rows, -1)
            key_at = lax.broadcasted_iota(jnp.int32, (rows, key.shape[0]), 1)
            allowed = jnp.logical_and(seg_ref[own, :] == all_ref[b], key_at <= at_ref[...])
            scores = jnp.where(allowed[None], scores, F32(-1e30))
            top = jnp.max(scores, axis=-1, keepdims=True)
            raised = jnp.exp(scores - top)
            weights = (raised * (1.0 / jnp.sum(raised, axis=-1, keepdims=True))).astype(BF16)
            weights = weights.reshape(heads * rows, -1)
            held[j] = weights
            put(j).start()
            mixed = jnp.dot(weights, value, preferred_element_type=F32)
            o_ref[own, columns] = side_by_side(mixed, rows).astype(BF16)
            return carry

        lax.fori_loop(0, self.batch * groups, step, 0)
        wo_copy.wait()

        def out_tile(t, carry):
            at = pl.ds(pl.multiple_of(t * 256, 256), 256)
            h_ref[:, at] = x_ref[:, at] + lax.dot_general(
                o_ref[...], wo[at, :], (((1,), (1,)), ((), ())), preferred_element_type=F32
            )
            return carry

        def norm_block(i, carry):
            at = pl.ds(pl.multiple_of(i * 32, 32), 32)
            value = h_ref[at, :]
            inv_rms = lax.rsqrt(jnp.mean(value * value, axis=-1, keepdims=True) + NORM_EPS)
            next_ref[at, :] = (value * inv_rms * gain_ref[...]).astype(BF16)
            return carry

        def finish():
            lax.fori_loop(0, wo.shape[0] // 256, out_tile, 0)
            lax.fori_loop(0, h_ref.shape[0] // 32, norm_block, 0)

        for k in range(2, max(self.n_t, last + 1)):
            if k < self.n_t:
                stage(3, k)
            if k == 2:
                finish()
            if k <= last:
                advance(1, k)
                advance(2, k)
        for j in range(self.batch * groups):
            put(j).wait()


def attend_back_kernel(do_ref, q_ref, kv_ref, p_ref, table_ref, dq_ref, dkv_ref):
    rows = q_ref.shape[0]
    kv = kv_ref[...].reshape(-1, 2 * HD)
    key, value = kv[:, :HD], kv[:, HD:]
    query, grad = stacked(q_ref[...]), stacked(do_ref[...])
    weights_b = p_ref[0, 0]
    weights = weights_b.astype(F32)
    product = weights * lax.dot_general(grad, value, (((1,), (1,)), ((), ())), preferred_element_type=F32)
    total = jnp.sum(product, axis=-1, keepdims=True)
    grad_scores = ((product - weights * total) * (1.0 / math.sqrt(HD))).astype(BF16)
    grad_query = side_by_side(jnp.dot(grad_scores, key, preferred_element_type=F32), rows)
    table = table_ref[:, :384]
    for j in range(q_ref.shape[1] // 128):
        at = slice(128 * j, 128 * j + 128)
        dq_ref[:, at] = turn(grad_query[:, at], table, -1.0).astype(BF16)
    over_rows = (((0,), (0,)), ((), ()))
    pair = jnp.concatenate(
        [
            lax.dot_general(query, grad_scores, over_rows, preferred_element_type=F32),
            lax.dot_general(grad, weights_b, over_rows, preferred_element_type=F32),
        ],
        axis=0,
    )
    dkv_ref[...] = pair.T.astype(BF16).reshape(dkv_ref.shape)


def attend_back(grad, q, kv, weights, table, heads):
    batch, groups, _, span = weights.shape
    rows = q.shape[0] // batch
    n_t = kv.shape[0]
    q_spec = pl.BlockSpec((rows, heads * HD), lambda b, g: (b, g))
    kv_spec = pl.BlockSpec((n_t, rows, 2 * HD), lambda b, g: (0, b, g))
    return pl.pallas_call(
        attend_back_kernel,
        grid=(batch, groups),
        out_shape=[jax.ShapeDtypeStruct(q.shape, BF16), jax.ShapeDtypeStruct(kv.shape, BF16)],
        in_specs=[
            q_spec,
            q_spec,
            kv_spec,
            pl.BlockSpec((1, 1, heads * rows, span), lambda b, g: (b, g, 0, 0)),
            pl.BlockSpec((rows, table.shape[1]), lambda b, g: (b, 0)),
        ],
        out_specs=[q_spec, kv_spec],
    )(grad, q, kv, weights, table)


def pair_sum_kernel(n_t, parts_ref, table_ref, out_ref, landed, send_sem, recv_sem):
    me = lax.axis_index("tensor")
    barrier = pltpu.get_barrier_semaphore()
    for r in range(1, n_t):
        pl.semaphore_signal(barrier, inc=1, device_id={"tensor": (me + r) % n_t}, device_id_type=MESH)
    pl.semaphore_wait(barrier, n_t - 1)

    def copy(r):
        other = (me + r) % n_t
        return pltpu.make_async_remote_copy(
            src_ref=parts_ref.at[other],
            dst_ref=landed.at[n_t - r],
            send_sem=send_sem.at[r],
            recv_sem=recv_sem.at[n_t - r],
            device_id={"tensor": other},
            device_id_type=MESH,
        )

    for r in range(1, n_t):
        copy(r).start()
    for r in range(1, n_t):
        other = (me + r) % n_t
        pltpu.make_async_remote_copy(
            src_ref=landed.at[r],
            dst_ref=landed.at[r],
            send_sem=send_sem.at[r],
            recv_sem=recv_sem.at[r],
            device_id={"tensor": other},
            device_id_type=MESH,
        ).wait_recv()
    table = table_ref[:, 384:]
    for j in range(out_ref.shape[1] // 128):
        at = slice(128 * j, 128 * j + 128)
        total = parts_ref[me, :, at].astype(F32)
        for r in range(1, n_t):
            total = total + landed[r, :, at].astype(F32)
        out_ref[:, at] = turn(total, table, -1.0).astype(BF16)
    for r in range(1, n_t):
        copy(r).wait_send()


def pair_sum(parts, table, n_t, ident):
    vmem = pl.BlockSpec(memory_space=pltpu.VMEM)
    return pl.pallas_call(
        functools.partial(pair_sum_kernel, n_t),
        out_shape=jax.ShapeDtypeStruct(parts.shape[1:], BF16),
        in_specs=[vmem, vmem],
        out_specs=vmem,
        scratch_shapes=[
            pltpu.VMEM(parts.shape, BF16),
            pltpu.SemaphoreType.DMA((n_t,)),
            pltpu.SemaphoreType.DMA((n_t,)),
        ],
        compiler_params=pltpu.CompilerParams(collective_id=ident, has_side_effects=True),
    )(parts, table)


def rope_tables(segments, start, rows):
    own = lax.dynamic_slice_in_dim(segments, start, rows, axis=1)
    earlier = jnp.sum((segments[:, None, :] < own[:, :, None]).astype(jnp.int32), axis=2)
    position = (start + jnp.arange(rows, dtype=jnp.int32)[None, :] - earlier).astype(F32)
    frequency = jnp.exp(jnp.arange(HD // 2, dtype=F32) * (-2.0 * math.log(10000.0) / HD))
    angles = (position[..., None] * frequency).reshape(-1, HD // 2)
    cosine, sine = jnp.cos(angles), jnp.sin(angles)
    zero, one = jnp.zeros_like(sine), jnp.ones_like(sine)
    columns = [cosine] * 4 + [-sine, zero] * 2 + [zero, sine] * 2
    columns += [cosine] * 2 + [one] * 2 + [-sine, zero, zero, zero] + [zero, sine, zero, zero]
    return own, jnp.concatenate(columns, axis=1)


def norm_forward(rows, gain):
    inv_rms = lax.rsqrt(jnp.mean(rows * rows, axis=-1, keepdims=True) + NORM_EPS)
    return (rows * inv_rms * gain).astype(BF16), inv_rms


def norm_backward(rows, inv_rms, gain, upstream):
    weighted = upstream * gain
    back = inv_rms * weighted - rows * (inv_rms * inv_rms * inv_rms) * jnp.mean(
        weighted * rows, axis=-1, keepdims=True
    )
    return back, jnp.sum(upstream * rows * inv_rms, axis=0)


def dot_nt(left, right):
    return lax.dot_general(left, right, (((1,), (1,)), ((), ())), preferred_element_type=F32)


def dot_tn(left, right):
    return lax.dot_general(left, right, (((0,), (0,)), ((), ())), preferred_element_type=F32)


def dot_nn(left, right):
    return jnp.dot(left, right, preferred_element_type=F32)


def dp_scatter(x):
    return lax.psum_scatter(x, "dp", scatter_dimension=0, tiled=True)


def body(
    heads, layer_input, segments, gain_attn, w_qkv, w_out_t, gain_mlp, w_gate_up, w_down_t, cotangent
):
    n_dp, n_t = lax.axis_size("dp"), lax.axis_size("tensor")
    me_t = lax.axis_index("tensor")
    batch, rows, width = layer_input.shape
    tokens = batch * rows
    shard_d = w_qkv.shape[0]
    q_cols = heads * HD
    parts = Cube(n_dp).parts

    x = layer_input.reshape(tokens, width)
    grad_in = cotangent.reshape(tokens, width)

    grad_b = grad_in.astype(BF16)
    w_local = w_qkv.reshape(shard_d, -1)
    gains = jnp.concatenate([gain_attn, gain_mlp]).astype(F32)
    gains = jnp.pad(gains, (0, 8 * parts * 128 - gains.shape[0])).reshape(8 * parts, 128)
    sources = [w_local[:, :q_cols], w_local[:, q_cols:], w_out_t, gains, grad_b[: tokens // 2]]
    first = Gather(
        ["zd", "zd", "zd", "d", "z"], [0, 0, 0, 0, 1], [s.shape for s in sources], n_t, n_dp, 1
    )
    wq, wkv, wo, gains, grad_low = first(*sources)
    gains = gains.reshape(n_dp, -1)[:, : 2 * shard_d].reshape(n_dp, 2, shard_d)
    g_attn = gains[:, 0].reshape(1, width)
    g_mlp = gains[:, 1].reshape(1, width)

    own_seg, table = rope_tables(segments, me_t * rows, rows)
    own_at = me_t * rows + jnp.arange(rows, dtype=jnp.int32)
    normed_attn, scale_attn = norm_forward(x, g_attn)
    pairs = rope(dot_nn(normed_attn, wkv), table)
    groups = pairs.shape[1] // (2 * HD)
    work = Attend(Cube(n_dp), n_t, batch, rows, heads, groups, segments.shape[1], width)
    second = [pairs, w_gate_up.reshape(shard_d, -1), w_down_t, grad_b[tokens // 2 :]]
    second = Gather(["z", "d", "d", "z"], [0, 0, 0, 1], [s.shape for s in second], n_t, n_dp, 2, work)(
        *second,
        given=(normed_attn, table, x, g_mlp, own_seg.reshape(-1, 1), own_at[:, None], segments[:, None, :], wq, wo),
    )
    pairs, gu_w, down_w, grad_high, query, mixed, residual, normed_mlp, weights = second
    weights = weights.reshape((batch, groups) + weights.shape[1:])

    scale_mlp = norm_forward(residual, g_mlp)[1]
    mlp_rows, grad_rows, hidden, grad_gu, back_parts, *out_parts = Mlp(n_t, 3)(
        normed_mlp, grad_low, grad_high, gu_w, down_w
    )
    flat = n_t * tokens
    down_part = dot_tn(grad_rows.reshape(flat, width), hidden.reshape(flat, -1)).astype(BF16)
    down_part, mlp_rows = lax.optimization_barrier((down_part, mlp_rows))
    down_grad = dp_scatter(down_part)
    gate_up_part = dot_tn(mlp_rows.reshape(flat, width), grad_gu.reshape(flat, -1)).astype(BF16)
    gate_up_part, back_parts = lax.optimization_barrier((gate_up_part, back_parts))
    gate_up_grad = dp_scatter(gate_up_part)

    grad_normed = jnp.sum(back_parts.astype(F32), axis=0)
    back_mlp, gain_mlp_part = norm_backward(residual, scale_mlp, g_mlp, grad_normed)
    grad_resid = grad_in + back_mlp
    resid_b = grad_resid.astype(BF16)

    out_grad = dot_tn(resid_b, mixed).astype(BF16)
    grad_mixed = dot_nn(resid_b, wo).astype(BF16)
    grad_query, grad_pairs = attend_back(grad_mixed, query, pairs, weights, table, heads)
    grad_pairs = pair_sum(grad_pairs, table, n_t, 5)
    grad_pairs, out_parts = lax.optimization_barrier((grad_pairs, out_parts))
    moved = [out_parts[0]] + [
        lax.ppermute(out_parts[r], "tensor", [(i, (i + r) % n_t) for i in range(n_t)]) for r in range(1, n_t)
    ]
    q_grad = dot_tn(normed_attn, grad_query).astype(BF16)
    kv_grad = dot_tn(normed_attn, grad_pairs).astype(BF16)
    grad_normed_attn = dot_nt(grad_query, wq) + dot_nt(grad_pairs, wkv)
    back_attn, gain_attn_part = norm_backward(x, scale_attn, g_attn, grad_normed_attn)
    input_grad = grad_resid + back_attn

    gain_parts = jnp.stack([gain_attn_part.reshape(n_dp, -1), gain_mlp_part.reshape(n_dp, -1)], axis=1)
    gain_parts = gain_parts.reshape(n_dp, -1)
    gain_parts = jnp.pad(gain_parts, ((0, 0), (0, 8 * parts * 128 - gain_parts.shape[1]))).reshape(-1, 128)
    q_grad, kv_grad, out_grad, gain_grads = Scatter(["dz", "dz", "dz", "da"], [1, 1, 1, 1], n_t, n_dp, 4)(
        q_grad, kv_grad, out_grad, gain_parts
    )
    gain_grads = gain_grads.reshape(-1)[: 2 * shard_d]
    gain_first, gain_second = gain_grads[:shard_d], gain_grads[shard_d:]
    down_grad, gate_up_grad, q_grad, moved = lax.optimization_barrier((down_grad, gate_up_grad, q_grad, moved))
    output = residual
    for part in moved:
        output = output + part.astype(F32)
    gate_up_grad = gate_up_grad.astype(F32)
    qkv_grad = jnp.concatenate([q_grad, kv_grad], axis=1)
    return (
        output.reshape(layer_input.shape),
        input_grad.reshape(layer_input.shape),
        gain_first,
        qkv_grad.reshape(w_qkv.shape),
        out_grad,
        gain_second,
        gate_up_grad.reshape(w_gate_up.shape),
        down_grad.astype(F32),
    )


def solution(mesh):
    placed = (
        P("dp", "tensor", None),
        P("dp", None),
        P("dp"),
        P("dp", "tensor", None),
        P("dp", "tensor"),
        P("dp"),
        P("dp", None, "tensor"),
        P("dp", "tensor"),
        P("dp", "tensor", None),
    )

    def whole(*args):
        heads = args[3].shape[2] // HD - 2
        return jax.shard_map(
            functools.partial(body, heads),
            mesh=mesh,
            in_specs=placed,
            out_specs=(placed[0], placed[0], P("dp"), placed[3], placed[4], P("dp"), placed[6], placed[7]),
            check_vma=False,
        )(*args)

    return whole
```

```python
import functools
import math

import jax
import jax.numpy as jnp
from jax import lax
from jax.experimental import pallas as pl
from jax.experimental.pallas import tpu as pltpu
from jax.sharding import PartitionSpec as P

HD = 64
NORM_EPS = 1e-05
F32 = jnp.float32
BF16 = jnp.bfloat16
MESH = pl.DeviceIdType.MESH
LATE = 2


class Cube:
    def __init__(self, size):
        self.size = size
        self.bits = size.bit_length() - 1
        assert 1 << self.bits == size and self.bits >= 1
        self.shape = (2,) * self.bits
        outer = list(range(1, self.bits))
        self.steps = len(outer)
        self.parts = max(1, self.steps)
        self.orders = [outer[p:] + outer[:p] for p in range(self.parts)]

    def own(self, bit):
        return lax.axis_index("dp") // (1 << bit) % 2

    def partner(self, bit):
        return lax.axis_index("dp") + (1 << bit) * (1 - 2 * self.own(bit))

    def index(self, free, flipped=()):
        spots = []
        for bit in reversed(range(self.bits)):
            if bit in free:
                spots.append(slice(None))
            else:
                spots.append(1 - self.own(bit) if bit in flipped else self.own(bit))
        return tuple(spots)

    def cuts(self, rows):
        count = rows // self.parts
        return [pl.ds(part * count, count) for part in range(self.parts)]

    def move(self, step, part):
        if step == self.steps:
            return tuple(range(1, self.bits)), 0
        return tuple(self.orders[part][:step]), self.orders[part][step]

    def keys(self, step):
        return [(step, part) for part in range(self.parts if step < self.steps else 1)]

    def row(self, key):
        return key[0] * self.parts + key[1]


class Gather:
    def __init__(self, kinds, late, shapes, n_t, n_dp, ident, work=None):
        self.work = work
        self.more_in, self.more_out = (work.more_in, work.more_out) if work else (0, 0)
        self.kinds, self.late, self.shapes = kinds, late, shapes
        self.n_t, self.cube, self.ident = n_t, Cube(n_dp), ident
        self.ticks = [[("own", 0)]] + [[("up", k), ("down", k)] for k in range(1, n_t)]
        self.insts = [inst for tick in self.ticks for inst in tick]
        self.uses_dp = any("d" in kind for kind in kinds)
        self.uses_z = any("z" in kind for kind in kinds)
    def out_shape(self, a):
        rows, cols = self.shapes[a]
        kind = self.kinds[a]
        if kind == "z":
            return (self.n_t, rows, cols)
        return self.cube.shape + (rows, cols * (self.n_t if "z" in kind else 1))

    def place(self, ref, a, z, free=(), flipped=(), part=None):
        rows, cols = self.shapes[a]
        kind = self.kinds[a]
        if kind == "z":
            return ref.at[z]
        span = pl.ds(0, rows) if part is None else self.cube.cuts(rows)[part]
        width = pl.ds(pl.multiple_of(z * cols, cols), cols) if "z" in kind else pl.ds(0, cols)
        return ref.at[self.cube.index(free, flipped) + (span, width)]

    def kernel(self, *refs):
        count = len(self.kinds)
        more_in, more_out = self.more_in, self.more_out
        srcs, given = refs[:count], refs[count : count + more_in]
        refs = refs[count + more_in :]
        dests, wanted, scratch = refs[:count], refs[count : count + more_out], refs[count + more_out + 5 :]
        own_sem, z_send, z_recv, d_send, d_recv = refs[count + more_out : count + more_out + 5]
        n_t, cube = self.n_t, self.cube
        me_t = lax.axis_index("tensor")
        main = [a for a in range(count) if not self.late[a]]
        tail = [a for a in range(count) if self.late[a]]

        barrier = pltpu.get_barrier_semaphore()
        if self.uses_dp:
            for bit in range(cube.bits):
                pl.semaphore_signal(barrier, inc=1, device_id={"dp": cube.partner(bit)}, device_id_type=MESH)
        peers = self.n_t - 1 if self.uses_z else 0
        for r in range(peers):
            pl.semaphore_signal(barrier, inc=1, device_id={"tensor": (me_t + 1 + r) % n_t}, device_id_type=MESH)
        pl.semaphore_wait(barrier, peers + (cube.bits if self.uses_dp else 0))

        def own_copy(a):
            return pltpu.make_async_copy(srcs[a], self.place(dests[a], a, me_t), own_sem.at[a])

        for a in range(count):
            own_copy(a).start()

        def piece_of(inst):
            way, k = inst
            return me_t if way == "own" else me_t - k if way == "up" else me_t + k

        def exists(inst, fn):
            way, k = inst
            if way == "own":
                fn()
            elif way == "up":
                pl.when(me_t >= k)(fn)
            else:
                pl.when(me_t + k < n_t)(fn)

        def z_copy(a, way, k, src):
            piece = me_t - (k - 1) if way == "up" else me_t + (k - 1)
            index = 2 * (k - 1) + (way == "down")
            dest = self.place(dests[a], a, piece)
            return pltpu.make_async_remote_copy(
                src_ref=dest if src is None else src,
                dst_ref=dest,
                send_sem=z_send.at[a, index],
                recv_sem=z_recv.at[a, index],
                device_id={"tensor": me_t + 1 if way == "up" else me_t - 1},
                device_id_type=MESH,
            )

        def z_cond(way, k):
            return (
                jnp.logical_and(me_t >= k - 1, me_t < n_t - 1)
                if way == "up"
                else jnp.logical_and(me_t + (k - 1) < n_t, me_t > 0)
            )

        def z_start(a, inst):
            way, k = inst
            for out_way in ("up", "down") if way == "own" else (way,):
                if k + 1 < n_t:

                    @pl.when(z_cond(out_way, k + 1))
                    def _():
                        z_copy(a, out_way, k + 1, srcs[a] if way == "own" else None).start()

        def z_arrive(a, inst):
            way, k = inst
            if way != "own":
                index = 2 * (k - 1) + (way == "down")
                dest = self.place(dests[a], a, piece_of(inst))
                pltpu.make_async_remote_copy(
                    src_ref=dest,
                    dst_ref=dest,
                    send_sem=z_send.at[a, index],
                    recv_sem=z_recv.at[a, index],
                    device_id={"tensor": me_t},
                    device_id_type=MESH,
                ).wait_recv()

        def d_copy(a, inst, key, incoming=False):
            free, bit = cube.move(*key)
            part = key[1] if key[0] < cube.steps else None
            spot = self.place(dests[a], a, piece_of(inst), free, (bit,) if incoming else (), part)
            sem = (a, self.insts.index(inst), cube.row(key))
            return pltpu.make_async_remote_copy(
                src_ref=spot,
                dst_ref=spot,
                send_sem=d_send.at[sem],
                recv_sem=d_recv.at[sem],
                device_id={"dp": cube.partner(bit)},
                device_id_type=MESH,
            )

        def d_advance(a, inst, stage):
            if stage == 0 and inst[0] == "own":
                own_copy(a).wait()
            if stage > 0:
                for key in cube.keys(stage - 1):
                    d_copy(a, inst, key, True).wait_recv()
            if stage <= cube.steps:
                for key in cube.keys(stage):
                    d_copy(a, inst, key).start()

        def in_dp(a, inst):
            return "d" in self.kinds[a] and (inst[0] == "own" or "z" in self.kinds[a])

        def stage(a, now):
            for inst in self.ticks[now]:

                def move(inst=inst):
                    z_arrive(a, inst)
                    z_start(a, inst)

                exists(inst, move)

        def plan():
            z_main = [a for a in main if "z" in self.kinds[a]]
            z_tail = [a for a in tail if "z" in self.kinds[a]]
            length = n_t if self.uses_z else 1
            total = max(length + cube.steps + 2, 2 * length + 1)
            for now in range(total):
                for inst in self.ticks[now] if now < length else ():
                    def arrive(inst=inst):
                        for a in z_main:
                            z_arrive(a, inst)
                            z_start(a, inst)
                        for a in main:
                            if in_dp(a, inst):
                                d_advance(a, inst, 0)

                    exists(inst, arrive)
                late_now = now - length + LATE
                if 0 <= late_now < length and z_tail:
                    for inst in self.ticks[late_now]:
                        def arrive_late(inst=inst):
                            for a in z_tail:
                                z_arrive(a, inst)
                                z_start(a, inst)

                        exists(inst, arrive_late)
                for age in range(1, cube.steps + 2):
                    tick = now - age
                    for inst in self.ticks[tick] if 0 <= tick < length else ():
                        def advance(inst=inst, age=age):
                            for a in main:
                                if in_dp(a, inst):
                                    d_advance(a, inst, age)

                        exists(inst, advance)

        if self.work is not None:
            self.work(
                stage, lambda a, age: d_advance(a, ("own", 0), age), own_copy, given, dests, wanted, scratch
            )
        else:
            plan()

        for inst in self.insts:
            def drain(inst=inst):
                for a in main:
                    if in_dp(a, inst):
                        for stage in range(cube.steps + 1):
                            for key in cube.keys(stage):
                                d_copy(a, inst, key).wait_send()

            exists(inst, drain)
        for a in range(count):
            if "z" in self.kinds[a]:
                for k in range(1, n_t):
                    for way in ("up", "down"):

                        @pl.when(z_cond(way, k))
                        def _():
                            z_copy(a, way, k, srcs[a] if k == 1 else None).wait_send()

            if not in_dp(a, ("own", 0)) and not (self.work and a == 0):
                own_copy(a).wait()

    def __call__(self, *arrays, given=()):
        count, work = len(arrays), self.work
        vmem, anywhere = pl.BlockSpec(memory_space=pltpu.VMEM), pl.BlockSpec(memory_space=pl.ANY)
        n_z = max(1, 2 * (self.n_t - 1))
        rows = (self.cube.steps + 1) * self.cube.parts
        insts = len(self.insts) if self.uses_dp else 1
        outs = pl.pallas_call(
            self.kernel,
            out_shape=[jax.ShapeDtypeStruct(self.out_shape(a), arrays[a].dtype) for a in range(count)]
            + (work.out_shape if work else []),
            in_specs=[vmem] * count + (work.in_specs if work else []),
            out_specs=[vmem if work and a == 0 else anywhere for a in range(count)] + (work.out_specs if work else []),
            scratch_shapes=[
                pltpu.SemaphoreType.DMA((count,)),
                pltpu.SemaphoreType.DMA((count, n_z)),
                pltpu.SemaphoreType.DMA((count, n_z)),
                pltpu.SemaphoreType.DMA((count, insts, rows)),
                pltpu.SemaphoreType.DMA((count, insts, rows)),
            ]
            + (work.scratch if work else []),
            compiler_params=pltpu.CompilerParams(
                collective_id=self.ident, has_side_effects=True, vmem_limit_bytes=60 << 20
            ),
        )(*arrays, *given)
        return [
            out.reshape(-1, out.shape[-1]) if "d" in kind else out for out, kind in zip(outs, self.kinds)
        ] + list(outs[count:])


class Scatter:
    def __init__(self, kinds, pieces, n_t, n_dp, ident):
        self.kinds = kinds
        self.pieces = [n_t if kind == "dz" else count for kind, count in zip(kinds, pieces)]
        self.n_t, self.cube, self.ident = n_t, Cube(n_dp), ident

    def kernel(self, *refs):
        count = len(self.kinds)
        n_t, cube = self.n_t, self.cube
        grads, outs = refs[:count], refs[count : 2 * count]
        core_in, z_in = refs[2 * count : 3 * count], refs[3 * count : 4 * count]
        step_in = [refs[4 * count + a * cube.steps :][: cube.steps] for a in range(count)]
        d_send, d_recv, z_send, z_recv = refs[-4:]
        me_t = lax.axis_index("tensor")
        to_z = any(kind != "d" for kind in self.kinds)

        barrier = pltpu.get_barrier_semaphore()
        for bit in range(cube.bits):
            pl.semaphore_signal(barrier, inc=1, device_id={"dp": cube.partner(bit)}, device_id_type=MESH)
        if to_z:
            for r in range(1, n_t):
                pl.semaphore_signal(barrier, inc=1, device_id={"tensor": (me_t + r) % n_t}, device_id_type=MESH)
        pl.semaphore_wait(barrier, cube.bits + (n_t - 1 if to_z else 0))

        def columns(a, i):
            width = grads[a].shape[-1] // self.pieces[a]
            if self.kinds[a] == "dz":
                return pl.ds(pl.multiple_of((me_t + n_t - 1 - i) % n_t * width, width), width)
            return pl.ds(i * width, width)

        def blocks(a, i, key, flipped=()):
            free, bit = cube.move(*key)
            rows = grads[a].shape[-2]
            span = cube.cuts(rows)[key[1]] if key[0] < cube.steps else pl.ds(0, rows)
            return grads[a].at[cube.index(free, flipped) + (span, columns(a, i))]

        def mine(a, i):
            return grads[a].at[cube.index(()) + (pl.ds(0, grads[a].shape[-2]), columns(a, i))]

        def landing(a, i, key):
            step, part = key
            if step == cube.steps:
                return core_in[a].at[i]
            return step_in[a][step].at[i, part]

        def d_copy(a, i, key):
            free, bit = cube.move(*key)
            return pltpu.make_async_remote_copy(
                src_ref=blocks(a, i, key, (bit,)),
                dst_ref=landing(a, i, key),
                send_sem=d_send.at[a, i, cube.row(key)],
                recv_sem=d_recv.at[a, i, cube.row(key)],
                device_id={"dp": cube.partner(bit)},
                device_id_type=MESH,
            )

        def add(a, i, key):
            free, bit = cube.move(*key)
            source = landing(a, i, key)
            rows = source.shape[-2]
            block = 16 if rows % 16 == 0 else 8
            first = cube.cuts(grads[a].shape[-2])[key[1]].start if key[0] < cube.steps else 0
            for number in range(1 << len(free)):
                held = sorted(free, reverse=True)
                bits = {b: number >> (len(held) - 1 - j) & 1 for j, b in enumerate(held)}
                target = grads[a].at[tuple(bits.get(b, cube.own(b)) for b in reversed(range(cube.bits)))]
                given = source.at[tuple(bits[b] for b in held)]

                def one(j, carry):
                    at = pl.ds(pl.multiple_of(j * block, block), block)
                    spot = (pl.ds(pl.multiple_of(first + j * block, block), block), columns(a, i))
                    target[spot] = (target[spot].astype(F32) + given[at, :].astype(F32)).astype(target.dtype)
                    return carry

                lax.fori_loop(0, rows // block, one, 0)

        def z_copy(a, i):
            other = (me_t + n_t - 1 - i) % n_t
            return pltpu.make_async_remote_copy(
                src_ref=mine(a, i if self.kinds[a] == "dz" else 0),
                dst_ref=z_in[a].at[me_t],
                send_sem=z_send.at[a, i],
                recv_sem=z_recv.at[a, me_t],
                device_id={"tensor": other},
                device_id_type=MESH,
            )

        def z_wait(a, r):
            other = (me_t + r) % n_t
            pltpu.make_async_remote_copy(
                src_ref=z_in[a].at[other],
                dst_ref=z_in[a].at[other],
                send_sem=z_send.at[a, 0],
                recv_sem=z_recv.at[a, other],
                device_id={"tensor": other},
                device_id_type=MESH,
            ).wait_recv()

        def advance(a, i, age):
            if age > 0:
                for key in cube.keys(cube.steps + 1 - age):
                    d_copy(a, i, key).wait_recv()
                    add(a, i, key)
            if age <= cube.steps:
                for key in cube.keys(cube.steps - age):
                    d_copy(a, i, key).start()
                return
            kind = self.kinds[a]
            if kind == "d":
                outs[a][:, columns(a, i)] = mine(a, i)[...].astype(F32)
            elif kind == "dz":
                if i < n_t - 1:
                    z_copy(a, i).start()
            else:
                for r in range(n_t - 1):
                    z_copy(a, r).start()

        most = max(self.pieces)
        order = range(count)
        for a in order:
            advance(a, 0, 0)
        for now in range(most + cube.steps + 1):
            for a in order:
                if now + 1 < self.pieces[a]:
                    advance(a, now + 1, 0)
            for age in range(cube.steps + 1, 0, -1):
                i = now + 1 - age
                for a in order:
                    if 0 <= i < self.pieces[a]:
                        advance(a, i, age)
        for a in order:
            if self.kinds[a] == "dz":
                for r in range(1, n_t):
                    z_wait(a, r)
                own = mine(a, n_t - 1)
                block = 16

                def total(j, carry, a=a, own=own):
                    at = pl.ds(pl.multiple_of(j * block, block), block)
                    value = own[at, :].astype(F32)
                    for r in range(1, n_t):
                        value = value + z_in[a][(me_t + r) % n_t, at, :].astype(F32)
                    outs[a][at, :] = value
                    return carry

                lax.fori_loop(0, own.shape[0] // block, total, 0)
            elif self.kinds[a] == "da":
                z_in[a][me_t] = mine(a, 0)[...]
                for r in range(1, n_t):
                    z_wait(a, r)
                value = z_in[a][0]
                for z in range(1, n_t):
                    value = value + z_in[a][z]
                outs[a][...] = value
        for a in order:
            for i in range(self.pieces[a]):
                for step in range(cube.steps + 1):
                    for key in cube.keys(step):
                        d_copy(a, i, key).wait_send()
            if self.kinds[a] != "d":
                for i in range(n_t - 1):
                    z_copy(a, i).wait_send()

    def __call__(self, *grads):
        count = len(grads)
        cube, n_t = self.cube, self.n_t
        outs, core, step, z = [], [], [], []
        for grad, kind, pieces in zip(grads, self.kinds, self.pieces):
            rows, cols = grad.shape[0] // cube.size, grad.shape[1] // pieces
            outs.append(jax.ShapeDtypeStruct((rows, cols if kind == "dz" else grad.shape[1]), F32))
            core.append(pltpu.VMEM((pieces,) + (2,) * cube.steps + (rows, cols), grad.dtype))
            for k in range(cube.steps):
                step.append(pltpu.VMEM((pieces, cube.parts) + (2,) * k + (rows // cube.parts, cols), grad.dtype))
            slots = (1, 8, 128) if kind == "d" else (n_t, rows, cols)
            z.append(pltpu.VMEM(slots, grad.dtype))
        most = max(self.pieces)
        keys = (cube.steps + 1) * cube.parts
        grads = [grad.reshape(cube.shape + (-1, grad.shape[1])) for grad in grads]
        return pl.pallas_call(
            self.kernel,
            out_shape=outs,
            in_specs=[pl.BlockSpec(memory_space=pltpu.VMEM)] * count,
            out_specs=[pl.BlockSpec(memory_space=pltpu.VMEM)] * count,
            scratch_shapes=core
            + z
            + step
            + [
                pltpu.SemaphoreType.DMA((count, most, keys)),
                pltpu.SemaphoreType.DMA((count, most, keys)),
                pltpu.SemaphoreType.DMA((count, n_t)),
                pltpu.SemaphoreType.DMA((count, n_t)),
            ],
            compiler_params=pltpu.CompilerParams(
                collective_id=self.ident, has_side_effects=True, vmem_limit_bytes=60 << 20
            ),
        )(*grads)


class Mlp:
    def __init__(self, n_t, ident):
        self.n_t, self.ident = n_t, ident

    def kernel(
        self, rows_ref, low_ref, high_ref, gu_hbm, down_hbm, all_ref, grads_ref, hid_ref, dgu_ref, back_ref, *refs
    ):
        out_refs = refs[: self.n_t]
        (gu, down, held, dy, dh, hid, dgu, flat, back, out, own_sem, w_sem, dy_sem, put_sem, z_send, z_recv, b_send, b_recv) = refs[self.n_t :]
        n_t = self.n_t
        me = lax.axis_index("tensor")
        units = down.shape[1]
        width = rows_ref.shape[1]
        interior = jnp.logical_and(me > 0, me < n_t - 1)

        barrier = pltpu.get_barrier_semaphore()
        for r in range(1, n_t):
            pl.semaphore_signal(barrier, inc=1, device_id={"tensor": (me + r) % n_t}, device_id_type=MESH)
        down_copy = pltpu.make_async_copy(down_hbm, down, w_sem.at[0])
        down_copy.start()

        gu_copies = [
            pltpu.make_async_copy(
                gu_hbm.at[:, pl.ds(half * units + 128 * t, 128)],
                gu.at[:, pl.ds(256 * t + 128 * half, 128)],
                w_sem.at[1 + 2 * t + half],
            )
            for t in range(units // 128)
            for half in (0, 1)
        ]
        for copy in gu_copies:
            copy.start()
        own_copy = pltpu.make_async_copy(rows_ref, held.at[me], own_sem)
        own_copy.start()

        def order(i):
            low, high = me, n_t - 1 - me
            both = 2 * jnp.minimum(low, high)
            near = i <= both
            distance = jnp.where(near, (i + 1) // 2, i - both // 2)
            way = jnp.where(near, (i + 1) % 2, jnp.where(low > high, 0, 1))
            return distance, way, jnp.where(way == 0, me - distance, me + distance)

        def piece_of(i):
            return order(i)[2]

        def hop(distance, way, piece, src=None):
            index = 2 * (distance - 1) + way
            return pltpu.make_async_remote_copy(
                src_ref=held.at[piece] if src is None else src,
                dst_ref=held.at[piece],
                send_sem=z_send.at[index],
                recv_sem=z_recv.at[index],
                device_id={"tensor": me + 1 - 2 * way},
                device_id_type=MESH,
            )

        def may_send(distance, way):
            room = jnp.where(way == 0, n_t - 1 - me, me)
            behind = jnp.where(way == 0, me, n_t - 1 - me)
            return jnp.logical_and(room > 0, behind >= distance - 1)

        def arrive(i):
            distance, way, piece = order(i)
            hop(distance, way, piece).wait_recv()

            @pl.when(may_send(distance + 1, way))
            def _():
                hop(distance + 1, way, piece).start()

        def dy_copies(i):
            part = low_ref.shape[1]
            return [
                pltpu.make_async_copy(ref.at[piece_of(i)], dy.at[i % 2, pl.ds(k * part, part), :], dy_sem.at[i % 2, k])
                for k, ref in enumerate((low_ref, high_ref))
            ]

        def dy_keep(i):
            return pltpu.make_async_copy(dy.at[i % 2], grads_ref.at[piece_of(i)], dy_sem.at[2, 0])

        def puts(i):
            piece, slot = piece_of(i), i % 2
            return [
                pltpu.make_async_copy(hid.at[slot], hid_ref.at[piece], put_sem.at[slot, 0]),
                pltpu.make_async_copy(flat.at[slot], dgu_ref.at[piece], put_sem.at[slot, 1]),
            ]

        def out_put(i, r=0):
            return pltpu.make_async_copy(out.at[i % 2], out_refs[r], put_sem.at[i % 2, 2])

        def put_start(i):
            for put in puts(i):
                put.start()
            for r in range(n_t):

                @pl.when((piece_of(i) - me + n_t) % n_t == r)
                def _():
                    out_put(i, r).start()

        def put_wait(i):
            for put in puts(i):
                put.wait()
            out_put(i).wait()

        def keep(i):
            return pltpu.make_async_copy(held.at[piece_of(i)], all_ref.at[piece_of(i)], own_sem)

        def back_copy(i):
            piece = piece_of(i)
            return pltpu.make_async_remote_copy(
                src_ref=back.at[i],
                dst_ref=back_ref.at[me],
                send_sem=b_send.at[i],
                recv_sem=b_recv.at[me],
                device_id={"tensor": piece},
                device_id_type=MESH,
            )

        for copy in dy_copies(0):
            copy.start()
        pl.semaphore_wait(barrier, n_t - 1)
        for way in (0, 1):

            @pl.when(may_send(1, way))
            def _():
                hop(1, way, me, rows_ref).start()

        own_copy.wait()
        down_copy.wait()
        wide = units // 256

        def chunk(i, carry):
            slot = i % 2
            piece = piece_of(i)

            @pl.when(jnp.logical_and(i > 0, jnp.logical_not(interior)))
            def _():
                arrive(i)

            @pl.when(jnp.logical_and(i == 1, interior))
            def _():
                arrive(i)

            @pl.when(jnp.logical_and(jnp.logical_and(i > 0, i + 1 < n_t), interior))
            def _():
                arrive(i + 1)

            @pl.when(i + 1 < n_t)
            def _():
                for copy in dy_copies(i + 1):
                    copy.start()

            @pl.when(i >= 2)
            def _():
                put_wait(i - 2)

            for copy in dy_copies(i):
                copy.wait()
            keep(i).start()
            dy_keep(i).start()

            def grad_tile(t, c):
                at = pl.ds(pl.multiple_of(t * 256, 256), 256)
                dh[:, at] = jnp.dot(dy[slot], down[:, at], preferred_element_type=F32)
                return c

            lax.fori_loop(0, wide, grad_tile, 0)
            if units % 256:
                dh[:, wide * 256 :] = jnp.dot(dy[slot], down[:, wide * 256 :], preferred_element_type=F32)

            @pl.when(i == 0)
            def _():
                for copy in gu_copies:
                    copy.wait()

            def unit_tile(t, c):
                at = pl.ds(pl.multiple_of(t * 128, 128), 128)
                pair = jnp.dot(held[piece], gu[:, pl.ds(pl.multiple_of(t * 256, 256), 256)], preferred_element_type=F32)
                gate, up = pair[:, :128], pair[:, 128:]
                sigmoid = jax.nn.sigmoid(gate)
                active = gate * sigmoid
                grad = dh[:, at]
                hid[slot, :, at] = (active * up).astype(BF16)
                first = (grad * up * sigmoid * (1.0 + gate * (1.0 - sigmoid))).astype(BF16)
                second = (grad * active).astype(BF16)
                dgu[slot, :, pl.ds(pl.multiple_of(t * 256, 128), 128)] = first
                dgu[slot, :, pl.ds(pl.multiple_of(t * 256 + 128, 128), 128)] = second
                flat[slot, :, at] = first
                flat[slot, :, pl.ds(pl.multiple_of(units + t * 128, 128), 128)] = second
                return c

            lax.fori_loop(0, units // 128, unit_tile, 0)

            def back_tile(j, c):
                at = pl.ds(pl.multiple_of(j * 256, 256), 256)
                value = lax.dot_general(dgu[slot], gu[at, :], (((1,), (1,)), ((), ())), preferred_element_type=F32)
                back[i, :, at] = value.astype(BF16)
                return c

            lax.fori_loop(0, width // 256, back_tile, 0)

            @pl.when(i > 0)
            def _():
                back_copy(i).start()

            def out_tile(j, c):
                at = pl.ds(pl.multiple_of(j * 256, 256), 256)
                value = lax.dot_general(hid[slot], down[at, :], (((1,), (1,)), ((), ())), preferred_element_type=F32)
                out[slot, :, at] = value.astype(BF16)
                return c

            lax.fori_loop(0, width // 256, out_tile, 0)
            put_start(i)
            keep(i).wait()
            dy_keep(i).wait()
            return carry

        lax.fori_loop(0, n_t, chunk, 0)
        mine = pltpu.make_async_copy(back.at[0], back_ref.at[me], own_sem)
        mine.start()
        for i in range(max(0, n_t - 2), n_t):
            put_wait(i)
        for r in range(1, n_t):
            other = (me + r) % n_t
            pltpu.make_async_remote_copy(
                src_ref=back_ref.at[other],
                dst_ref=back_ref.at[other],
                send_sem=b_send.at[0],
                recv_sem=b_recv.at[other],
                device_id={"tensor": other},
                device_id_type=MESH,
            ).wait_recv()
        mine.wait()
        for i in range(1, n_t):
            back_copy(i).wait_send()
        for k in range(1, n_t):
            for way in (0, 1):

                @pl.when(may_send(k, way))
                def _():
                    hop(k, way, me, rows_ref).wait_send()

    def __call__(self, rows, low, high, w_gu, w_down):
        n_t = self.n_t
        tokens, width = rows.shape
        units = w_down.shape[1]
        hops = max(1, 2 * (n_t - 1))
        any_spec = pl.BlockSpec(memory_space=pl.ANY)

        def held(*shape):
            return pltpu.VMEM(shape, BF16)

        def put(cols, *lead):
            return jax.ShapeDtypeStruct(lead + (tokens, cols), BF16)

        return pl.pallas_call(
            self.kernel,
            out_shape=[put(width, n_t), put(width, n_t), put(units, n_t), put(2 * units, n_t), put(width, n_t)] + [put(width)] * n_t,
            in_specs=[pl.BlockSpec(memory_space=pltpu.VMEM)] + [any_spec] * 4,
            out_specs=[any_spec] * (5 + n_t),
            scratch_shapes=[
                held(width, 2 * units),
                held(width, units),
                held(n_t, tokens, width),
                held(2, tokens, width),
                pltpu.VMEM((tokens, units), F32),
                held(2, tokens, units),
                held(2, tokens, 2 * units),
                held(2, tokens, 2 * units),
                held(n_t, tokens, width),
                held(2, tokens, width),
                pltpu.SemaphoreType.DMA,
                pltpu.SemaphoreType.DMA((1 + units // 64,)),
                pltpu.SemaphoreType.DMA((3, 2)),
                pltpu.SemaphoreType.DMA((2, 3)),
                pltpu.SemaphoreType.DMA((hops,)),
                pltpu.SemaphoreType.DMA((hops,)),
                pltpu.SemaphoreType.DMA((n_t,)),
                pltpu.SemaphoreType.DMA((n_t,)),
            ],
            compiler_params=pltpu.CompilerParams(
                collective_id=self.ident, has_side_effects=True, vmem_limit_bytes=60 << 20
            ),
        )(rows, low, high, w_gu, w_down)


def turn(x, table, sign):
    cosine, low, high = table[:, :128], table[:, 128:256], table[:, 256:]
    return x * cosine + sign * (pltpu.roll(x, 96, 1) * low + pltpu.roll(x, 32, 1) * high)


def rope_kernel(kv_ref, table_ref, kvo_ref):
    for j in range(kv_ref.shape[1] // 128):
        at = slice(128 * j, 128 * j + 128)
        kvo_ref[:, at] = turn(kv_ref[:, at], table_ref[:, 384:], 1.0).astype(BF16)


def rope(kv, table):
    vmem = pl.BlockSpec(memory_space=pltpu.VMEM)
    return pl.pallas_call(
        rope_kernel, out_shape=jax.ShapeDtypeStruct(kv.shape, BF16), in_specs=[vmem, vmem], out_specs=vmem
    )(kv, table)


def stacked(x):
    return jnp.concatenate([x[:, HD * h : HD * (h + 1)] for h in range(x.shape[1] // HD)], axis=0)


def side_by_side(x, rows):
    return jnp.concatenate([x[rows * h : rows * (h + 1)] for h in range(x.shape[0] // rows)], axis=1)


class Attend:
    more_in, more_out = 9, 5

    def __init__(self, cube, n_t, batch, rows, heads, groups, span, width):
        self.cube, self.n_t, self.batch, self.rows, self.heads, self.groups = cube, n_t, batch, rows, heads, groups
        steps, tokens, inner = batch * groups, batch * rows, groups * heads * HD
        self.out_shape = [
            jax.ShapeDtypeStruct((tokens, inner), BF16),
            jax.ShapeDtypeStruct((tokens, inner), BF16),
            jax.ShapeDtypeStruct((tokens, width), F32),
            jax.ShapeDtypeStruct((tokens, width), BF16),
            jax.ShapeDtypeStruct((steps, heads * rows, span), BF16),
        ]
        self.out_specs = [pl.BlockSpec(memory_space=pltpu.VMEM)] * 4 + [pl.BlockSpec(memory_space=pl.ANY)]
        self.scratch = [
            pltpu.VMEM((steps, heads * rows, span), BF16),
            pltpu.SemaphoreType.DMA((steps,)),
            pltpu.VMEM((width, inner), BF16),
            pltpu.VMEM((width, inner), BF16),
            pltpu.SemaphoreType.DMA((2,)),
        ]
        vmem = pl.BlockSpec(memory_space=pltpu.VMEM)
        self.in_specs = [vmem] * 7 + [pl.BlockSpec(memory_space=pl.ANY)] * 2

    def __call__(self, stage, advance, own_copy, given, dests, wanted, scratch):
        n_ref, table_ref, x_ref, gain_ref, seg_ref, at_ref, all_ref, wq_hbm, wo_hbm = given
        q_ref, o_ref, h_ref, next_ref, p_ref = wanted
        held, sem, wq, wo, w_sem = scratch
        kv_ref = dests[0]
        rows, heads, groups = self.rows, self.heads, self.groups
        last = self.cube.steps + 1
        wq_copy = pltpu.make_async_copy(wq_hbm, wq, w_sem.at[0])
        wo_copy = pltpu.make_async_copy(wo_hbm, wo, w_sem.at[1])
        stage(0, 0)
        wq_copy.start()
        advance(1, 0)
        advance(2, 0)
        wo_copy.start()

        def query_tile(t, carry):
            at = pl.ds(pl.multiple_of(t * 256, 256), 256)
            value = jnp.dot(n_ref[...], wq[:, at], preferred_element_type=F32)
            for half in (0, 1):
                place = pl.ds(pl.multiple_of(t * 256 + half * 128, 128), 128)
                q_ref[:, place] = turn(value[:, 128 * half : 128 * half + 128], table_ref[:, :384], 1.0).astype(BF16)
            return carry

        half = wq.shape[1] // 512
        if self.n_t > 1:
            stage(0, 1)
        stage(3, 0)
        wq_copy.wait()
        lax.fori_loop(0, half, query_tile, 0)
        if self.n_t > 2:
            stage(0, 2)
        advance(1, 1)
        lax.fori_loop(half, 2 * half, query_tile, 0)
        for tick in range(3, self.n_t):
            stage(0, tick)
        own_copy(0).wait()
        advance(2, 1)
        if self.n_t > 1:
            stage(3, 1)

        def put(j):
            return pltpu.make_async_copy(held.at[j], p_ref.at[j], sem.at[j])

        def step(j, carry):
            b, g = j // groups, j % groups
            own = pl.ds(pl.multiple_of(b * rows, rows), rows)
            columns = pl.ds(pl.multiple_of(g * heads * HD, 128), heads * HD)
            kv = kv_ref[:, own, pl.ds(pl.multiple_of(g * 2 * HD, 2 * HD), 2 * HD)].reshape(-1, 2 * HD)
            key, value = kv[:, :HD], kv[:, HD:]
            scores = lax.dot_general(
                stacked(q_ref[own, columns]), key, (((1,), (1,)), ((), ())), preferred_element_type=F32
            )
            scores = (scores * (1.0 / math.sqrt(HD))).reshape(heads, rows, -1)
            key_at = lax.broadcasted_iota(jnp.int32, (rows, key.shape[0]), 1)
            allowed = jnp.logical_and(seg_ref[own, :] == all_ref[b], key_at <= at_ref[...])
            scores = jnp.where(allowed[None], scores, F32(-1e30))
            top = jnp.max(scores, axis=-1, keepdims=True)
            raised = jnp.exp(scores - top)
            weights = (raised * (1.0 / jnp.sum(raised, axis=-1, keepdims=True))).astype(BF16)
            weights = weights.reshape(heads * rows, -1)
            held[j] = weights
            put(j).start()
            mixed = jnp.dot(weights, value, preferred_element_type=F32)
            o_ref[own, columns] = side_by_side(mixed, rows).astype(BF16)
            return carry

        lax.fori_loop(0, self.batch * groups, step, 0)
        wo_copy.wait()

        def out_tile(t, carry):
            at = pl.ds(pl.multiple_of(t * 256, 256), 256)
            h_ref[:, at] = x_ref[:, at] + lax.dot_general(
                o_ref[...], wo[at, :], (((1,), (1,)), ((), ())), preferred_element_type=F32
            )
            return carry

        def norm_block(i, carry):
            at = pl.ds(pl.multiple_of(i * 32, 32), 32)
            value = h_ref[at, :]
            inv_rms = lax.rsqrt(jnp.mean(value * value, axis=-1, keepdims=True) + NORM_EPS)
            next_ref[at, :] = (value * inv_rms * gain_ref[...]).astype(BF16)
            return carry

        def finish():
            lax.fori_loop(0, wo.shape[0] // 256, out_tile, 0)
            lax.fori_loop(0, h_ref.shape[0] // 32, norm_block, 0)

        for k in range(2, max(self.n_t, last + 1)):
            if k < self.n_t:
                stage(3, k)
            if k == 2:
                finish()
            if k <= last:
                advance(1, k)
                advance(2, k)
        for j in range(self.batch * groups):
            put(j).wait()


def attend_back_kernel(do_ref, q_ref, kv_ref, p_ref, table_ref, dq_ref, dkv_ref):
    rows = q_ref.shape[0]
    kv = kv_ref[...].reshape(-1, 2 * HD)
    key, value = kv[:, :HD], kv[:, HD:]
    query, grad = stacked(q_ref[...]), stacked(do_ref[...])
    weights_b = p_ref[0, 0]
    weights = weights_b.astype(F32)
    product = weights * lax.dot_general(grad, value, (((1,), (1,)), ((), ())), preferred_element_type=F32)
    total = jnp.sum(product, axis=-1, keepdims=True)
    grad_scores = ((product - weights * total) * (1.0 / math.sqrt(HD))).astype(BF16)
    grad_query = side_by_side(jnp.dot(grad_scores, key, preferred_element_type=F32), rows)
    table = table_ref[:, :384]
    for j in range(q_ref.shape[1] // 128):
        at = slice(128 * j, 128 * j + 128)
        dq_ref[:, at] = turn(grad_query[:, at], table, -1.0).astype(BF16)
    over_rows = (((0,), (0,)), ((), ()))
    pair = jnp.concatenate(
        [
            lax.dot_general(query, grad_scores, over_rows, preferred_element_type=F32),
            lax.dot_general(grad, weights_b, over_rows, preferred_element_type=F32),
        ],
        axis=0,
    )
    dkv_ref[...] = pair.T.astype(BF16).reshape(dkv_ref.shape)


def attend_back(grad, q, kv, weights, table, heads):
    batch, groups, _, span = weights.shape
    rows = q.shape[0] // batch
    n_t = kv.shape[0]
    q_spec = pl.BlockSpec((rows, heads * HD), lambda b, g: (b, g))
    kv_spec = pl.BlockSpec((n_t, rows, 2 * HD), lambda b, g: (0, b, g))
    return pl.pallas_call(
        attend_back_kernel,
        grid=(batch, groups),
        out_shape=[jax.ShapeDtypeStruct(q.shape, BF16), jax.ShapeDtypeStruct(kv.shape, BF16)],
        in_specs=[
            q_spec,
            q_spec,
            kv_spec,
            pl.BlockSpec((1, 1, heads * rows, span), lambda b, g: (b, g, 0, 0)),
            pl.BlockSpec((rows, table.shape[1]), lambda b, g: (b, 0)),
        ],
        out_specs=[q_spec, kv_spec],
    )(grad, q, kv, weights, table)


def pair_sum_kernel(n_t, parts_ref, table_ref, out_ref, landed, send_sem, recv_sem):
    me = lax.axis_index("tensor")
    barrier = pltpu.get_barrier_semaphore()
    for r in range(1, n_t):
        pl.semaphore_signal(barrier, inc=1, device_id={"tensor": (me + r) % n_t}, device_id_type=MESH)
    pl.semaphore_wait(barrier, n_t - 1)

    def copy(r):
        other = (me + r) % n_t
        return pltpu.make_async_remote_copy(
            src_ref=parts_ref.at[other],
            dst_ref=landed.at[n_t - r],
            send_sem=send_sem.at[r],
            recv_sem=recv_sem.at[n_t - r],
            device_id={"tensor": other},
            device_id_type=MESH,
        )

    for r in range(1, n_t):
        copy(r).start()
    for r in range(1, n_t):
        other = (me + r) % n_t
        pltpu.make_async_remote_copy(
            src_ref=landed.at[r],
            dst_ref=landed.at[r],
            send_sem=send_sem.at[r],
            recv_sem=recv_sem.at[r],
            device_id={"tensor": other},
            device_id_type=MESH,
        ).wait_recv()
    table = table_ref[:, 384:]
    for j in range(out_ref.shape[1] // 128):
        at = slice(128 * j, 128 * j + 128)
        total = parts_ref[me, :, at].astype(F32)
        for r in range(1, n_t):
            total = total + landed[r, :, at].astype(F32)
        out_ref[:, at] = turn(total, table, -1.0).astype(BF16)
    for r in range(1, n_t):
        copy(r).wait_send()


def pair_sum(parts, table, n_t, ident):
    vmem = pl.BlockSpec(memory_space=pltpu.VMEM)
    return pl.pallas_call(
        functools.partial(pair_sum_kernel, n_t),
        out_shape=jax.ShapeDtypeStruct(parts.shape[1:], BF16),
        in_specs=[vmem, vmem],
        out_specs=vmem,
        scratch_shapes=[
            pltpu.VMEM(parts.shape, BF16),
            pltpu.SemaphoreType.DMA((n_t,)),
            pltpu.SemaphoreType.DMA((n_t,)),
        ],
        compiler_params=pltpu.CompilerParams(collective_id=ident, has_side_effects=True),
    )(parts, table)


def rope_tables(segments, start, rows):
    own = lax.dynamic_slice_in_dim(segments, start, rows, axis=1)
    earlier = jnp.sum((segments[:, None, :] < own[:, :, None]).astype(jnp.int32), axis=2)
    position = (start + jnp.arange(rows, dtype=jnp.int32)[None, :] - earlier).astype(F32)
    frequency = jnp.exp(jnp.arange(HD // 2, dtype=F32) * (-2.0 * math.log(10000.0) / HD))
    angles = (position[..., None] * frequency).reshape(-1, HD // 2)
    cosine, sine = jnp.cos(angles), jnp.sin(angles)
    zero, one = jnp.zeros_like(sine), jnp.ones_like(sine)
    columns = [cosine] * 4 + [-sine, zero] * 2 + [zero, sine] * 2
    columns += [cosine] * 2 + [one] * 2 + [-sine, zero, zero, zero] + [zero, sine, zero, zero]
    return own, jnp.concatenate(columns, axis=1)


def norm_forward(rows, gain):
    inv_rms = lax.rsqrt(jnp.mean(rows * rows, axis=-1, keepdims=True) + NORM_EPS)
    return (rows * inv_rms * gain).astype(BF16), inv_rms


def norm_backward(rows, inv_rms, gain, upstream):
    weighted = upstream * gain
    back = inv_rms * weighted - rows * (inv_rms * inv_rms * inv_rms) * jnp.mean(
        weighted * rows, axis=-1, keepdims=True
    )
    return back, jnp.sum(upstream * rows * inv_rms, axis=0)


def dot_nt(left, right):
    return lax.dot_general(left, right, (((1,), (1,)), ((), ())), preferred_element_type=F32)


def dot_tn(left, right):
    return lax.dot_general(left, right, (((0,), (0,)), ((), ())), preferred_element_type=F32)


def dot_nn(left, right):
    return jnp.dot(left, right, preferred_element_type=F32)


def dp_scatter(x):
    return lax.psum_scatter(x, "dp", scatter_dimension=0, tiled=True)


def body(
    heads, layer_input, segments, gain_attn, w_qkv, w_out_t, gain_mlp, w_gate_up, w_down_t, cotangent
):
    n_dp, n_t = lax.axis_size("dp"), lax.axis_size("tensor")
    me_t = lax.axis_index("tensor")
    batch, rows, width = layer_input.shape
    tokens = batch * rows
    shard_d = w_qkv.shape[0]
    q_cols = heads * HD
    parts = Cube(n_dp).parts

    x = layer_input.reshape(tokens, width)
    grad_in = cotangent.reshape(tokens, width)

    grad_b = grad_in.astype(BF16)
    w_local = w_qkv.reshape(shard_d, -1)
    gains = jnp.concatenate([gain_attn, gain_mlp]).astype(F32)
    gains = jnp.pad(gains, (0, 8 * parts * 128 - gains.shape[0])).reshape(8 * parts, 128)
    sources = [w_local[:, :q_cols], w_local[:, q_cols:], w_out_t, gains, grad_b[: tokens // 2]]
    first = Gather(
        ["zd", "zd", "zd", "d", "z"], [0, 0, 0, 0, 1], [s.shape for s in sources], n_t, n_dp, 1
    )
    wq, wkv, wo, gains, grad_low = first(*sources)
    gains = gains.reshape(n_dp, -1)[:, : 2 * shard_d].reshape(n_dp, 2, shard_d)
    g_attn = gains[:, 0].reshape(1, width)
    g_mlp = gains[:, 1].reshape(1, width)

    own_seg, table = rope_tables(segments, me_t * rows, rows)
    own_at = me_t * rows + jnp.arange(rows, dtype=jnp.int32)
    normed_attn, scale_attn = norm_forward(x, g_attn)
    pairs = rope(dot_nn(normed_attn, wkv), table)
    groups = pairs.shape[1] // (2 * HD)
    work = Attend(Cube(n_dp), n_t, batch, rows, heads, groups, segments.shape[1], width)
    second = [pairs, w_gate_up.reshape(shard_d, -1), w_down_t, grad_b[tokens // 2 :]]
    second = Gather(["z", "d", "d", "z"], [0, 0, 0, 1], [s.shape for s in second], n_t, n_dp, 2, work)(
        *second,
        given=(normed_attn, table, x, g_mlp, own_seg.reshape(-1, 1), own_at[:, None], segments[:, None, :], wq, wo),
    )
    pairs, gu_w, down_w, grad_high, query, mixed, residual, normed_mlp, weights = second
    weights = weights.reshape((batch, groups) + weights.shape[1:])

    scale_mlp = norm_forward(residual, g_mlp)[1]
    mlp_rows, grad_rows, hidden, grad_gu, back_parts, *out_parts = Mlp(n_t, 3)(
        normed_mlp, grad_low, grad_high, gu_w, down_w
    )
    flat = n_t * tokens
    gate_up_part = dot_tn(mlp_rows.reshape(flat, width), grad_gu.reshape(flat, -1)).astype(BF16)
    gate_up_part, grad_rows = lax.optimization_barrier((gate_up_part, grad_rows))
    gate_up_grad = dp_scatter(gate_up_part)
    down_part = dot_tn(grad_rows.reshape(flat, width), hidden.reshape(flat, -1)).astype(BF16)
    down_part, back_parts = lax.optimization_barrier((down_part, back_parts))
    down_grad = dp_scatter(down_part)

    grad_normed = jnp.sum(back_parts.astype(F32), axis=0)
    back_mlp, gain_mlp_part = norm_backward(residual, scale_mlp, g_mlp, grad_normed)
    grad_resid = grad_in + back_mlp
    resid_b = grad_resid.astype(BF16)

    out_grad = dot_tn(resid_b, mixed).astype(BF16)
    grad_mixed = dot_nn(resid_b, wo).astype(BF16)
    grad_query, grad_pairs = attend_back(grad_mixed, query, pairs, weights, table, heads)
    grad_pairs = pair_sum(grad_pairs, table, n_t, 5)
    grad_pairs, out_parts = lax.optimization_barrier((grad_pairs, out_parts))
    moved = [out_parts[0]] + [
        lax.ppermute(out_parts[r], "tensor", [(i, (i + r) % n_t) for i in range(n_t)]) for r in range(1, n_t)
    ]
    q_grad = dot_tn(normed_attn, grad_query).astype(BF16)
    kv_grad = dot_tn(normed_attn, grad_pairs).astype(BF16)
    grad_normed_attn = dot_nt(grad_query, wq) + dot_nt(grad_pairs, wkv)
    back_attn, gain_attn_part = norm_backward(x, scale_attn, g_attn, grad_normed_attn)
    input_grad = grad_resid + back_attn

    gain_parts = jnp.stack([gain_attn_part.reshape(n_dp, -1), gain_mlp_part.reshape(n_dp, -1)], axis=1)
    gain_parts = gain_parts.reshape(n_dp, -1)
    gain_parts = jnp.pad(gain_parts, ((0, 0), (0, 8 * parts * 128 - gain_parts.shape[1]))).reshape(-1, 128)
    q_grad, kv_grad, out_grad, gain_grads = Scatter(["dz", "dz", "dz", "da"], [1, 1, 1, 1], n_t, n_dp, 4)(
        q_grad, kv_grad, out_grad, gain_parts
    )
    gain_grads = gain_grads.reshape(-1)[: 2 * shard_d]
    gain_first, gain_second = gain_grads[:shard_d], gain_grads[shard_d:]
    down_grad, gate_up_grad, q_grad, moved = lax.optimization_barrier((down_grad, gate_up_grad, q_grad, moved))
    output = residual
    for part in moved:
        output = output + part.astype(F32)
    gate_up_grad = gate_up_grad.astype(F32)
    qkv_grad = jnp.concatenate([q_grad, kv_grad], axis=1)
    return (
        output.reshape(layer_input.shape),
        input_grad.reshape(layer_input.shape),
        gain_first,
        qkv_grad.reshape(w_qkv.shape),
        out_grad,
        gain_second,
        gate_up_grad.reshape(w_gate_up.shape),
        down_grad.astype(F32),
    )


def solution(mesh):
    placed = (
        P("dp", "tensor", None),
        P("dp", None),
        P("dp"),
        P("dp", "tensor", None),
        P("dp", "tensor"),
        P("dp"),
        P("dp", None, "tensor"),
        P("dp", "tensor"),
        P("dp", "tensor", None),
    )

    def whole(*args):
        heads = args[3].shape[2] // HD - 2
        return jax.shard_map(
            functools.partial(body, heads),
            mesh=mesh,
            in_specs=placed,
            out_specs=(placed[0], placed[0], P("dp"), placed[3], placed[4], P("dp"), placed[6], placed[7]),
            check_vma=False,
        )(*args)

    return whole
```
